256 devices in a mesh: dev: 64 (over z, y, core), rep: 4 (over x).
Axes of the slice: x: 4, y: 4, z: 8, core: 2. Of those that a mesh axis runs over, the one named last changes fastest.
Arguments:
- features: bfloat16 [262144, 256], P(('dev', 'rep')), may hold values from -6 to 6
- history: bfloat16 [262144, 256], P(('dev', 'rep')), may hold values from -6 to 6
- new_owner: int32 [256, 64], P(('dev', 'rep')), may hold values from 0 to 63, as said below
- pull_rows: int32 [262144], P(('dev', 'rep')), may hold values from 0 to 1023
- occupancy: int32 [2048, 16], P(('dev', 'rep')), may hold values from 0 to 1, as said below
- adj_local: bfloat16 [262144, 1024], P(('dev', 'rep')), may hold values from -0.125 to 0.125
- adj_boundary: bfloat16 [262144, 1024], P(('dev', 'rep')), may hold values from -0.125 to 0.125
- w_first: bfloat16 [256, 256], replicated, may hold values from -0.375 to 0.375
- bias_first: float32 [256], replicated, may hold values from -3 to 3
- w_second: bfloat16 [256, 256], replicated, may hold values from -0.375 to 0.375
- cotangent: bfloat16 [262144, 256], P(('dev', 'rep')), may hold values from -24 to 24
Outputs:
- hidden: bfloat16 [262144, 256], P(('dev', 'rep'))
- output: bfloat16 [262144, 256], P(('dev', 'rep'))
- w_second_grad: float32 [256, 256], replicated
The draws below stay inside these ranges and needn't reach their ends.
Inputs may be any that keep to these rules, and one draw needn't show every extreme that they name: Each row of new_owner is a permutation of 0 to 63. `occupancy`: tile flags of 0 or 1.
All inputs are finite; a program needn't handle non-finite values.
Results may differ from the reference program's by a relative error of at most 0.0061.
Values may be sent and summed in bfloat16 or wider, within the bound.
No kernel may reach another device: no remote copies, remote signals or barrier semaphores. Data moves between devices by JAX's collectives and lax.ppermute only.
A program may use at most 64 MiB of HBM per device.

```python
import jax
import jax.numpy as jnp
from jax import lax

F = 256
ROWS_DEV = 1024
PULL_DEV = 1024
NODES = 262144
N_DEV = 64
N_REP = 4


def draw_new_owner(key, part):
    keys = jax.random.split(jax.random.fold_in(key, 11), N_DEV * N_REP)

    def shuffle(single):
        return jax.random.permutation(single, N_DEV)
    return jax.vmap(shuffle)(keys).astype(jnp.int32)


def draw_occupancy(key, part):
    tile_rows = ROWS_DEV // 128
    tile_cols = (ROWS_DEV + PULL_DEV) // 128
    total = N_DEV * N_REP
    first, second = jax.random.split(jax.random.fold_in(key, 23))
    level = jax.random.randint(first, (total, 1, 1), 1, 5)
    rolled = jax.random.randint(second, (total, tile_rows, tile_cols), 0, 4)
    return (rolled < level).astype(jnp.int32).reshape(total * tile_rows, tile_cols)


def set_ends(entries, stream_key, smallest, top_value):
    spot = [jax.random.randint(jax.random.fold_in(stream_key, axis), (), 0, length) for axis, length in enumerate(entries.shape)]
    longest = entries.shape.index(max(entries.shape))
    next_to = spot[:longest] + [(spot[longest] + 1) % entries.shape[longest]] + spot[longest + 1:]
    return entries.at[tuple(spot)].set(smallest).at[tuple(next_to)].set(top_value)


def with_spikes(values, rng, source, target, shards_of, factor):
    def block_of(dim):
        return (jnp.arange(values.shape[dim]) // (values.shape[dim] // shards_of)).reshape((-1,) + (1,) * (values.ndim - 1 - dim))

    first = jax.random.permutation(rng, shards_of)[block_of(target)]
    other_side = (block_of(target) + shards_of // 2) % shards_of
    return jnp.where((block_of(source) == first) | (block_of(source) == other_side), factor * values, values)


def block_scale(stream_key, dims, shards, low, high):
    def one(dim, shards_of):
        draws = jax.random.uniform(jax.random.fold_in(jax.random.fold_in(stream_key, 6), dim), (shards_of,), jnp.float32, low / len(shards), high / len(shards))
        return jnp.repeat(jnp.exp(draws), dims[dim] // shards_of).reshape((-1,) + (1,) * (len(dims) - dim - 1))

    loudness = one(*shards[0])
    for cut in shards[1:]:
        loudness = loudness * one(*cut)
    return loudness


def bell_draw(stream_key, dims, scale, limit, cuts=(), kind=jnp.bfloat16):
    loudness = block_scale(stream_key, dims, cuts, -0.22, 0.18) if cuts else 1.0
    values = jax.random.normal(stream_key, dims, jnp.float32) * scale * loudness
    return jnp.minimum(jnp.maximum(values, -limit), limit).astype(kind)


def gaussian_with(stream_key, extent, scale, bound, cuts, heavy, kind=jnp.bfloat16):
    array = scale * jax.random.normal(stream_key, extent, jnp.float32)
    if cuts:
        array = array * block_scale(stream_key, extent, cuts, -0.22, 0.18)
    return jnp.clip(with_spikes(array, jax.random.fold_in(stream_key, 3), *heavy), -bound, bound).astype(kind)


def setup_inputs(seed: int = 0) -> dict:
    splits = jax.random.split(jax.random.key(seed), 12)
    features = bell_draw(splits[0], (NODES, F), 1.0, 6.0, ((0, 256),))
    history = bell_draw(splits[1], (NODES, F), 1.0, 6.0, ((0, 256),))
    new_owner = draw_new_owner(jax.random.fold_in(splits[11], 71), 0)
    pull_rows = set_ends(jax.random.randint(splits[3], (N_DEV * N_REP * PULL_DEV,), 0, ROWS_DEV), jax.random.fold_in(splits[3], 1), 0, ROWS_DEV - 1).astype(jnp.int32)
    occupancy = draw_occupancy(jax.random.fold_in(splits[11], 71), 0)
    adj_local = bell_draw(splits[5], (NODES, ROWS_DEV), (ROWS_DEV + PULL_DEV) ** -0.5, 0.125, ((0, 256),))
    adj_boundary = bell_draw(splits[6], (NODES, PULL_DEV), (ROWS_DEV + PULL_DEV) ** -0.5, 0.125, ((0, 256),))
    w_first = bell_draw(splits[7], (F, F), F ** -0.5, 0.375)
    bias_first = bell_draw(splits[8], (F,), 0.5, 3.0, (), jnp.float32)
    w_second = bell_draw(splits[9], (F, F), F ** -0.5, 0.375)
    cotangent = gaussian_with(splits[10], (NODES, F), 1.0, 24.0, ((0, 256),), (0, 1, 256, 6.0))
    return dict(features=features, history=history, new_owner=new_owner, pull_rows=pull_rows, occupancy=occupancy, adj_local=adj_local, adj_boundary=adj_boundary, w_first=w_first, bias_first=bias_first, w_second=w_second, cotangent=cotangent)


def expand(occupied):
    return jnp.repeat(jnp.repeat(occupied, 128, axis=-2), 128, axis=-1).astype(jnp.bfloat16)


def reference(features, history, new_owner, pull_rows, occupancy, adj_local, adj_boundary, w_first, bias_first, w_second, cotangent):
    peer_count = N_DEV
    copies = N_REP
    height = ROWS_DEV
    breadth = F
    cluster = height // peer_count
    pulled = PULL_DEV
    per_peer = pulled // peer_count
    indices = jnp.arange(peer_count, dtype=jnp.int32)
    routes = new_owner.reshape(peer_count, copies, peer_count)
    matches = (routes[:, :, :, None] == indices).astype(jnp.int32)
    inverse = jnp.sum(matches * indices[:, None], axis=2).astype(jnp.int32)

    def migrate(values):
        blocks = values.reshape(peer_count, copies, peer_count, cluster, breadth)
        where_from = jnp.broadcast_to(inverse[:, :, :, None, None], blocks.shape)
        arrived = jnp.take_along_axis(blocks, where_from, axis=2)
        return arrived.transpose(2, 1, 0, 3, 4).reshape(peer_count, copies, height, breadth)

    own_x = migrate(features)
    own_h = migrate(history)
    wanted = pull_rows.reshape(peer_count, copies, pulled)
    owners = jnp.arange(pulled, dtype=jnp.int32) // per_peer
    flat_rows = (owners[None, None, :] * height + wanted).astype(jnp.int32)
    replica_ids = jnp.arange(copies, dtype=jnp.int32)[None, :, None]

    def fetch_remote(values):
        spread = values.transpose(1, 0, 2, 3).reshape(copies, peer_count * height, breadth)
        return spread[replica_ids, flat_rows]

    def scatter(partial_value):
        summed = jnp.zeros((copies, peer_count * height, breadth), jnp.float32)
        summed = summed.at[replica_ids, flat_rows].add(partial_value.astype(jnp.float32))
        summed = summed.reshape(copies, peer_count, height, breadth).transpose(1, 0, 2, 3)
        return summed.reshape(peer_count * copies * height, breadth)

    tile_mask = occupancy.reshape(peer_count * copies, height // 128, (height + pulled) // 128)
    local_adj = adj_local.reshape(peer_count * copies, height, height)
    edge_adj = adj_boundary.reshape(peer_count * copies, height, pulled)

    def layer_terms(owned, remote):
        def device(operands):
            owned_rows, theirs, local_tile, edge_tile, flags = operands
            full_mask = expand(flags)
            local_tile = local_tile * full_mask[:, :height]
            edge_tile = edge_tile * full_mask[:, height:]
            summed = jnp.dot(local_tile, owned_rows, preferred_element_type=jnp.float32)
            summed = summed + jnp.dot(edge_tile, theirs, preferred_element_type=jnp.float32)
            partial_value = lax.dot_general(edge_tile, owned_rows, (((0,), (0,)), ((), ())), preferred_element_type=jnp.float32)
            return summed, partial_value.astype(jnp.bfloat16)

        summed, partial_value = lax.map(device, (owned.reshape(-1, height, breadth), remote.reshape(-1, pulled, breadth), local_adj, edge_adj, tile_mask))
        return summed.reshape(-1, breadth), partial_value.reshape(peer_count, copies, pulled, breadth)

    summed_one, partial_one = layer_terms(own_x, fetch_remote(own_x))
    aggregate_one = (summed_one + scatter(partial_one)).astype(jnp.bfloat16)
    hidden = jnp.maximum(jnp.dot(aggregate_one, w_first, preferred_element_type=jnp.float32) + bias_first, 0.0).astype(jnp.bfloat16)
    summed_two, partial_two = layer_terms(hidden.reshape(peer_count, copies, height, breadth), fetch_remote(own_h))
    aggregate_two = (summed_two + scatter(partial_two)).astype(jnp.bfloat16)
    output = jnp.dot(aggregate_two, w_second, preferred_element_type=jnp.float32).astype(jnp.bfloat16)
    gradient = lax.dot_general(aggregate_two, cotangent, (((0,), (0,)), ((), ())), preferred_element_type=jnp.float32)
    return hidden, output, gradient
```

```python
import jax
import jax.numpy as jnp
from jax import lax
from jax.experimental import pallas as pl
from jax.experimental.pallas import tpu as pltpu
from jax.sharding import Mesh
from jax.sharding import PartitionSpec as P

CHIPS = ("dev_0", "dev_1")
DEV = ("dev_0", "dev_1", "dev_2")
DEV_REP = ("dev_0", "dev_1", "dev_2", "rep")
PEERS, SLOT, HALF, ROWS, F = 64, 16, 128, 1024, 256
STEP = 256

F32, BF16 = jnp.float32, jnp.bfloat16


def dot(a, b):
    return jnp.dot(a, b, preferred_element_type=F32)


def call(body, outs, operands, *, smem=0, scratch=(), flops=0, mib=24, name=None):
    specs = [
        pl.BlockSpec(memory_space=pltpu.SMEM if i < smem else pltpu.VMEM)
        for i in range(len(operands))
    ]
    moved = sum(a.size * a.dtype.itemsize for a in (*operands, *outs))
    return pl.pallas_call(
        body,
        out_shape=outs,
        in_specs=specs,
        out_specs=tuple(pl.BlockSpec(memory_space=pltpu.VMEM) for _ in outs),
        scratch_shapes=scratch,
        compiler_params=pltpu.CompilerParams(vmem_limit_bytes=mib << 20),
        cost_estimate=pl.CostEstimate(flops=flops, bytes_accessed=moved, transcendentals=0),
        name=name,
    )(*operands)


def shaped(*dims, dtype=BF16):
    return jax.ShapeDtypeStruct(dims, dtype)


def put(message, at, peers, value):
    count = value.shape[0] // SLOT
    message[peers, at : at + SLOT, :] = value[:, :HALF].reshape(count, SLOT, HALF)
    message[peers, at + SLOT : at + 2 * SLOT, :] = value[:, HALF:].reshape(count, SLOT, HALF)


def take(message, at, into):
    into[:, :HALF] = message[:, at : at + SLOT, :].reshape(ROWS, HALF)
    into[:, HALF:] = message[:, at + SLOT : at + 2 * SLOT, :].reshape(ROWS, HALF)


def send_clusters(owner, x, h, pulled, message):
    for j in range(PEERS):
        e = owner[0, j]
        rows = slice(j * SLOT, (j + 1) * SLOT)
        message[e, 0:16, :] = x[rows, :HALF]
        message[e, 16:32, :] = x[rows, HALF:]
        message[e, 32:48, :] = h[rows, :HALF]
        message[e, 48:64, :] = h[rows, HALF:]
    which = lax.broadcasted_iota(jnp.int32, (8, HALF), 0)
    for a in range(8):
        numbers = pulled[a : a + 1, :]
        high = (numbers // 32).astype(F32)
        low = (numbers % 32).astype(F32)
        tile = jnp.where(which == 0, high, jnp.where(which == 1, low, 0.0)).astype(BF16)
        for b in range(8):
            message[a * 8 + b, 64:72, :] = tile


def requested(me, message):
    tile = message[:, 64:72, :].astype(F32)
    numbers = 32.0 * tile[:, 0:1, :] + tile[:, 1:2, :]
    lane = lax.broadcasted_iota(jnp.int32, (PEERS, SLOT, HALF), 2)
    place = lax.broadcasted_iota(jnp.int32, (PEERS, SLOT, HALF), 1)
    mine = lane == (me % 8) * SLOT + place
    return jnp.sum(jnp.where(mine, numbers, 0.0), axis=2, keepdims=True).reshape(ROWS, 1)


def mask_tiles(occupied, local, edge, local_out, edge_out, flipped_out):
    for i in range(8):
        rows = slice(i * 128, (i + 1) * 128)
        for j in range(8):
            cols = slice(j * 128, (j + 1) * 128)
            part = local[rows, cols]
            local_out[rows, cols] = jnp.where(occupied[i, j] != 0, part, jnp.zeros_like(part))
            part = edge[rows, cols]
            part = jnp.where(occupied[i, 8 + j] != 0, part, jnp.zeros_like(part))
            edge_out[rows, cols] = part
            flipped_out[cols, rows] = part.T


def serve(me, message, flipped, own_x, reply, own_h):
    take(message, 0, own_x)
    take(message, 32, own_h)
    wanted = requested(me[0], message).astype(jnp.int32)
    for at in range(0, ROWS, STEP):
        rows, peers = slice(at, at + STEP), slice(at // SLOT, (at + STEP) // SLOT)
        column = lax.broadcasted_iota(jnp.int32, (STEP, ROWS), 1)
        select = (column == wanted[rows]).astype(BF16)
        put(reply, 0, peers, dot(select, own_x[...]).astype(BF16))
        put(reply, 64, peers, dot(select, own_h[...]).astype(BF16))
        put(reply, 32, peers, dot(flipped[rows, :], own_x[...]).astype(BF16))


def prepare(me, message, local, own_x, partial, gather):
    wanted = jnp.broadcast_to(requested(me[0], message), (ROWS, HALF))
    row = lax.broadcasted_iota(jnp.int32, (ROWS, HALF), 0).astype(F32)
    for a in range(8):
        cols = slice(a * HALF, (a + 1) * HALF)
        gather[:, cols] = (row == wanted[cols].T[0:1, :]).astype(BF16)
    for at in range(0, ROWS, STEP):
        rows = slice(at, at + STEP)
        partial[rows, :] = dot(local[rows, :], own_x[...])


def first_layer(message, partial, edge, gather, flipped, w, bias, hidden, push, far, pushed):
    take(message, 0, far)
    take(message, 32, pushed)
    for at in range(0, ROWS, STEP):
        rows = slice(at, at + STEP)
        total = partial[rows, :] + dot(edge[rows, :], far[...]) + dot(gather[rows, :], pushed[...])
        value = dot(total.astype(BF16), w[...]) + bias[...]
        hidden[rows, :] = jnp.maximum(value, 0.0).astype(BF16)
    for at in range(0, ROWS, STEP):
        rows, peers = slice(at, at + STEP), slice(at // SLOT, (at + STEP) // SLOT)
        put(push, 0, peers, dot(flipped[rows, :], hidden[...]).astype(BF16))


def second_terms(message, local, edge, hidden, partial, far):
    take(message, 64, far)
    for at in range(0, ROWS, STEP):
        rows = slice(at, at + STEP)
        partial[rows, :] = dot(local[rows, :], hidden[...]) + dot(edge[rows, :], far[...])


def second_layer(message, partial, gather, cotangent, aggregate, gradient, pushed):
    take(message, 0, pushed)
    for at in range(0, ROWS, STEP):
        rows = slice(at, at + STEP)
        total = partial[rows, :] + dot(gather[rows, :], pushed[...])
        aggregate[rows, :] = total.astype(BF16)
    gradient[...] = lax.dot_general(
        aggregate[...], cotangent[...], (((0,), (0,)), ((), ())), preferred_element_type=F32
    )


def exchange(message):
    return lax.all_to_all(message, DEV, split_axis=0, concat_axis=0, tiled=True)


def swapped(array, axis, mask):
    return lax.ppermute(array, axis, [(i, i ^ mask) for i in range(lax.axis_size(axis))])


def summed_everywhere(term):
    core = lax.axis_index("dev_2")
    halves = term.reshape(2, ROWS // 8, F)
    kept = lax.dynamic_index_in_dim(halves, core, 0, keepdims=False)
    sent = lax.dynamic_index_in_dim(halves, 1 - core, 0, keepdims=False)
    half = kept + swapped(sent, "dev_2", 1)
    tiles = lax.all_to_all(half.reshape(32, 4, F), CHIPS, split_axis=0, concat_axis=0, tiled=True)
    own = jnp.sum(tiles, axis=0)
    own = (own + swapped(own, "rep", 1)) + (swapped(own, "rep", 2) + swapped(own, "rep", 3))
    copies = jnp.broadcast_to(own[None], (32, 4, F))
    mine = lax.all_to_all(copies, CHIPS, split_axis=0, concat_axis=0, tiled=True).reshape(128, F)
    other = swapped(mine, "dev_2", 1)
    first = jnp.where(core == 0, mine, other)
    second = jnp.where(core == 0, other, mine)
    return jnp.concatenate([first, second], axis=0)


def body(
    features,
    history,
    new_owner,
    pull_rows,
    occupancy,
    adj_local,
    adj_boundary,
    w_first,
    bias_first,
    w_second,
    cotangent,
):
    me = lax.axis_index(DEV).astype(jnp.int32).reshape(1)
    wide = 2 * ROWS * ROWS * F
    nodes = pltpu.VMEM((ROWS, F), BF16)

    (message,) = call(
        send_clusters,
        (shaped(PEERS, 72, HALF),),
        (new_owner, features, history, pull_rows.reshape(8, 128)),
        smem=1,
        flops=ROWS * F,
        name="send_clusters",
    )
    local, edge, flipped = call(
        mask_tiles,
        (shaped(ROWS, ROWS),) * 3,
        (occupancy, adj_local, adj_boundary),
        smem=1,
        flops=wide,
        name="mask_tiles",
    )
    arrived = exchange(message)
    own_x, reply = call(
        serve,
        (shaped(ROWS, F), shaped(PEERS, 96, HALF)),
        (me, arrived, flipped),
        smem=1,
        scratch=(nodes,),
        flops=3 * wide,
        name="serve",
    )
    partial_one, gather = call(
        prepare,
        (shaped(ROWS, F, dtype=F32), shaped(ROWS, ROWS)),
        (me, arrived, local, own_x),
        smem=1,
        flops=wide,
        name="prepare",
    )
    answers = exchange(reply)
    hidden, push = call(
        first_layer,
        (shaped(ROWS, F), shaped(PEERS, 32, HALF)),
        (answers, partial_one, edge, gather, flipped, w_first, bias_first.reshape(1, F)),
        scratch=(nodes, nodes),
        flops=3 * wide,
        name="first_layer",
    )
    (partial_two,) = call(
        second_terms,
        (shaped(ROWS, F, dtype=F32),),
        (answers, local, edge, hidden),
        scratch=(nodes,),
        flops=2 * wide,
        name="second_terms",
    )
    pushed = exchange(push)
    aggregate, term = call(
        second_layer,
        (shaped(ROWS, F), shaped(F, F, dtype=F32)),
        (pushed, partial_two, gather, cotangent),
        scratch=(nodes,),
        flops=2 * wide,
        name="second_layer",
    )
    output = jnp.dot(aggregate, w_second, preferred_element_type=F32).astype(BF16)
    return (hidden, output, summed_everywhere(term))


def solution(mesh):
    finer = Mesh(
        mesh.devices.reshape(8, 4, 2, mesh.shape["rep"]), ("dev_0", "dev_1", "dev_2", "rep")
    )
    rows = P(DEV_REP, None)
    return jax.shard_map(
        body,
        mesh=finer,
        in_specs=(rows, rows, rows, P(DEV_REP), rows, rows, rows, P(), P(), P(), rows),
        out_specs=(rows, rows, P()),
        check_vma=False,
    )
```

```python
import jax
import jax.numpy as jnp
from jax import lax
from jax.experimental import pallas as pl
from jax.experimental.pallas import tpu as pltpu
from jax.sharding import Mesh
from jax.sharding import PartitionSpec as P

DEV = ("dev_0", "dev_1", "dev_2")
DEV_REP = ("dev_0", "dev_1", "dev_2", "rep")
PEERS, SLOT, HALF, ROWS, F = 64, 16, 128, 1024, 256
STEP = 512
VMEM = 67043328

F32, BF16 = jnp.float32, jnp.bfloat16


def dot(a, b):
    return jnp.dot(a, b, preferred_element_type=F32)


def call(body, kinds, outs, operands, *, own=(), copies=0, flops=0, room=0, name=None):
    spaces = {"s": pltpu.SMEM, "v": pltpu.VMEM, "h": pltpu.HBM}
    moved = sum(a.size * a.dtype.itemsize for a in (*operands, *outs))
    arrivals = (pltpu.SemaphoreType.DMA((copies,)),) if copies else ()
    specs = [pl.BlockSpec(memory_space=spaces[k]) for k in kinds]
    return pl.pallas_call(
        body,
        out_shape=outs,
        in_specs=specs[: len(operands)],
        out_specs=tuple(specs[len(operands) :]),
        scratch_shapes=(*own, *arrivals),
        compiler_params=pltpu.CompilerParams(vmem_limit_bytes=VMEM - room),
        cost_estimate=pl.CostEstimate(flops=flops, bytes_accessed=moved, transcendentals=0),
        name=name,
    )(*operands)


class Copies:
    def __init__(self, semaphores):
        self.semaphores, self.used = semaphores, 0

    def start(self, source, target):
        copy = pltpu.make_async_copy(source, target, self.semaphores.at[self.used])
        self.used += 1
        copy.start()
        return copy

    def unpack(self, message, at, into, peers=slice(None)):
        left = self.start(message.at[peers, at : at + SLOT, :], into.at[peers, :, 0:HALF])
        right = self.start(message.at[peers, at + SLOT : at + 2 * SLOT, :], into.at[peers, :, HALF:])
        return (left, right)


def wait(*copies):
    for copy in copies:
        copy.wait()


def shaped(*dims, dtype=BF16):
    return jax.ShapeDtypeStruct(dims, dtype)


def put(message, at, peers, value):
    count = value.shape[0] // SLOT
    message[peers, at : at + SLOT, :] = value[:, :HALF].reshape(count, SLOT, HALF)
    message[peers, at + SLOT : at + 2 * SLOT, :] = value[:, HALF:].reshape(count, SLOT, HALF)


def steps():
    for at in range(0, ROWS, STEP):
        yield slice(at, at + STEP), slice(at // SLOT, (at + STEP) // SLOT)


def flat(ref):
    return ref[...].reshape(ROWS, F)


def send_clusters(owner, x, h, pulled, message, owners, xs, hs, numbers, packed, sem):
    copies = Copies(sem)
    order = copies.start(owner, owners)
    first = copies.start(x, xs)
    rows_in = copies.start(pulled, numbers)
    second = copies.start(h, hs)
    which = lax.broadcasted_iota(jnp.int32, (8, HALF), 0)
    rows_in.wait()
    for a in range(8):
        line = numbers[a : a + 1, :]
        high = (line // 32).astype(F32)
        low = (line % 32).astype(F32)
        tile = jnp.where(which == 0, high, jnp.where(which == 1, low, 0.0)).astype(BF16)
        for b in range(8):
            packed[a * 8 + b, 64:72, :] = tile
    wait(order, first)
    for j in range(PEERS):
        e = owners[0, j]
        rows = slice(j * SLOT, (j + 1) * SLOT)
        packed[e, 0:16, :] = xs[rows, :HALF]
        packed[e, 16:32, :] = xs[rows, HALF:]
    out_x = copies.start(packed.at[:, 0:32, :], message.at[:, 0:32, :])
    second.wait()
    for j in range(PEERS):
        e = owners[0, j]
        rows = slice(j * SLOT, (j + 1) * SLOT)
        packed[e, 32:48, :] = hs[rows, :HALF]
        packed[e, 48:64, :] = hs[rows, HALF:]
    out_h = copies.start(packed.at[:, 32:72, :], message.at[:, 32:72, :])
    wait(out_x, out_h)


def requested(me, digits):
    tile = digits[...].astype(F32)
    numbers = 32.0 * tile[:, 0:1, :] + tile[:, 1:2, :]
    lane = lax.broadcasted_iota(jnp.int32, (PEERS, SLOT, HALF), 2)
    place = lax.broadcasted_iota(jnp.int32, (PEERS, SLOT, HALF), 1)
    mine = lane == (me % 8) * SLOT + place
    return jnp.sum(jnp.where(mine, numbers, 0.0), axis=2, keepdims=True).reshape(ROWS, 1)


def mask_tiles(occupied, local, edge, local_out, edge_out, flipped_out):
    for i in range(8):
        rows = slice(i * 128, (i + 1) * 128)
        for j in range(8):
            cols = slice(j * 128, (j + 1) * 128)
            part = local[rows, cols]
            local_out[rows, cols] = jnp.where(occupied[i, j] != 0, part, jnp.zeros_like(part))
            part = edge[rows, cols]
            part = jnp.where(occupied[i, 8 + j] != 0, part, jnp.zeros_like(part))
            edge_out[rows, cols] = part
            flipped_out[cols, rows] = part.T


def serve(
    me, message, flipped_far, own_far, reply_far, digits, own_x, own_h, flipped, reply, sem
):
    copies = Copies(sem)
    numbers = copies.start(message.at[:, 64:72, :], digits)
    first = copies.unpack(message, 0, own_x)
    second = copies.unpack(message, 32, own_h)
    third = copies.start(flipped_far, flipped)
    numbers.wait()
    wanted = requested(me[0], digits).astype(jnp.int32)
    wait(*first)
    out = [copies.start(own_x, own_far)]
    wait(*second)
    for rows, peers in steps():
        column = lax.broadcasted_iota(jnp.int32, (STEP, ROWS), 1)
        select = (column == wanted[rows]).astype(BF16)
        put(reply, 0, peers, dot(select, flat(own_x)).astype(BF16))
        put(reply, 64, peers, dot(select, flat(own_h)).astype(BF16))
    third.wait()
    for rows, peers in steps():
        put(reply, 32, peers, dot(flipped[rows, :], flat(own_x)).astype(BF16))
        out.append(copies.start(reply.at[peers], reply_far.at[peers]))
    wait(*out)


def prepare(me, message, local_far, own_far, partial, gather, digits, local, own_x, sem):
    copies = Copies(sem)
    numbers = copies.start(message.at[:, 64:72, :], digits)
    rest = (copies.start(own_far, own_x), copies.start(local_far, local))
    numbers.wait()
    wanted = jnp.broadcast_to(requested(me[0], digits), (ROWS, HALF))
    row = lax.broadcasted_iota(jnp.int32, (ROWS, HALF), 0).astype(F32)
    for a in range(8):
        cols = slice(a * HALF, (a + 1) * HALF)
        gather[:, cols] = (row == wanted[cols].T[0:1, :]).astype(BF16)
    wait(*rest)
    for rows, peers in steps():
        partial[rows, :] = dot(local[rows, :], flat(own_x))


def first_layer(
    message, partial_far, edge_far, gather_far, flipped_far, w_far, bias_far,
    hidden_far, push_far,
    far, pushed, partial, edge, gather, flipped, w, bias, hidden, push, sem,
):
    copies = Copies(sem)
    needed = (*copies.unpack(message, 0, far), *copies.unpack(message, 32, pushed))
    arriving = []
    for rows, peers in steps():
        arriving.append(
            [
                copies.start(whole.at[rows], part.at[rows])
                for whole, part in ((edge_far, edge), (gather_far, gather), (partial_far, partial))
            ]
        )
    small = (copies.start(w_far, w), copies.start(bias_far, bias))
    last = copies.start(flipped_far, flipped)
    wait(*needed)
    for (rows, peers), parts in zip(steps(), arriving):
        wait(*parts)
        total = partial[rows, :] + dot(edge[rows, :], flat(far)) + dot(gather[rows, :], flat(pushed))
        if rows.start == 0:
            wait(*small)
        value = dot(total.astype(BF16), w[...]) + bias[...]
        hidden[rows, :] = jnp.maximum(value, 0.0).astype(BF16)
    last.wait()
    out = [copies.start(hidden, hidden_far)]
    for rows, peers in steps():
        put(push, 0, peers, dot(flipped[rows, :], hidden[...]).astype(BF16))
        out.append(copies.start(push.at[peers], push_far.at[peers]))
    wait(*out)


def second_terms(
    message, local_far, edge_far, hidden_far, partial, far, local, edge, hidden, sem
):
    copies = Copies(sem)
    parts = [
        *copies.unpack(message, 64, far),
        copies.start(local_far, local),
        copies.start(edge_far, edge),
        copies.start(hidden_far, hidden),
    ]
    wait(*parts)
    for rows, peers in steps():
        partial[rows, :] = dot(local[rows, :], hidden[...]) + dot(edge[rows, :], flat(far))


def second_layer(
    message, partial_far, gather_far, cotangent_far,
    aggregate_far, gradient,
    pushed, partial, gather, cotangent, aggregate, sem,
):
    copies = Copies(sem)
    needed = copies.unpack(message, 0, pushed)
    arriving = []
    for rows, peers in steps():
        arriving.append(
            (
                copies.start(gather_far.at[rows], gather.at[rows]),
                copies.start(partial_far.at[rows], partial.at[rows]),
            )
        )
    last = copies.start(cotangent_far, cotangent)
    wait(*needed)
    for (rows, peers), parts in zip(steps(), arriving):
        wait(*parts)
        total = partial[rows, :] + dot(gather[rows, :], flat(pushed))
        aggregate[rows, :] = total.astype(BF16)
    out = copies.start(aggregate, aggregate_far)
    last.wait()
    gradient[...] = lax.dot_general(
        aggregate[...], cotangent[...], (((0,), (0,)), ((), ())), preferred_element_type=F32
    )
    out.wait()


def exchange(message):
    return lax.all_to_all(message, DEV, split_axis=0, concat_axis=0, tiled=True)


def swapped(array, axis, mask):
    return lax.ppermute(array, axis, [(i, i ^ mask) for i in range(lax.axis_size(axis))])


def summed_everywhere(term):
    group = ("dev_0", "dev_1", "rep")
    core = lax.axis_index("dev_2")
    halves = term.reshape(2, F // 2, F)
    kept = lax.dynamic_index_in_dim(halves, core, 0, keepdims=False)
    sent = lax.dynamic_index_in_dim(halves, 1 - core, 0, keepdims=False)
    half = kept + swapped(sent, "dev_2", 1)
    tiles = lax.all_to_all(half[:, None, :], group, split_axis=0, concat_axis=0, tiled=True)
    own = jnp.sum(tiles, axis=0, keepdims=True)
    copies = jnp.broadcast_to(own, (F // 2, 1, F))
    mine = lax.all_to_all(copies, group, split_axis=0, concat_axis=0, tiled=True)[:, 0, :]
    other = swapped(mine, "dev_2", 1)
    first = jnp.where(core == 0, mine, other)
    second = jnp.where(core == 0, other, mine)
    return jnp.concatenate([first, second], axis=0)


def body(
    features,
    history,
    new_owner,
    pull_rows,
    occupancy,
    adj_local,
    adj_boundary,
    w_first,
    bias_first,
    w_second,
    cotangent,
):
    me = lax.axis_index(DEV).astype(jnp.int32).reshape(1)
    wide = 2 * ROWS * ROWS * F
    nodes, square = pltpu.VMEM((ROWS, F), BF16), pltpu.VMEM((ROWS, ROWS), BF16)
    sums, peers = pltpu.VMEM((ROWS, F), F32), pltpu.VMEM((PEERS, SLOT, F), BF16)
    digits = pltpu.VMEM((PEERS, 8, HALF), BF16)
    count = ROWS // STEP

    def letters(rows):
        return pltpu.VMEM((PEERS, rows, HALF), BF16)

    (message,) = call(
        send_clusters,
        "hhhhh",
        (shaped(PEERS, 72, HALF),),
        (new_owner, features, history, pull_rows.reshape(8, 128)),
        own=(
            pltpu.SMEM((1, PEERS), jnp.int32),
            nodes,
            nodes,
            pltpu.VMEM((8, 128), jnp.int32),
            letters(72),
        ),
        copies=6,
        flops=ROWS * F,
        name="send_clusters",
    )
    local, edge, flipped = call(
        mask_tiles,
        "svvvvv",
        (shaped(ROWS, ROWS),) * 3,
        (occupancy, adj_local, adj_boundary),
        flops=wide,
        room=40 << 20,
        name="mask_tiles",
    )
    arrived = exchange(message)
    own_x, reply = call(
        serve,
        "shhhh",
        (shaped(PEERS, SLOT, F), shaped(PEERS, 96, HALF)),
        (me, arrived, flipped),
        own=(digits, peers, peers, square, letters(96)),
        copies=7 + count,
        flops=3 * wide,
        name="serve",
    )
    partial_one, gather = call(
        prepare,
        "shhhvv",
        (shaped(ROWS, F, dtype=F32), shaped(ROWS, ROWS)),
        (me, arrived, local, own_x),
        own=(digits, square, peers),
        copies=3,
        flops=wide,
        name="prepare",
    )
    answers = exchange(reply)
    hidden, push = call(
        first_layer,
        "hhhhhhhhh",
        (shaped(ROWS, F), shaped(PEERS, 32, HALF)),
        (answers, partial_one, edge, gather, flipped, w_first, bias_first.reshape(1, F)),
        own=(
            peers,
            peers,
            sums,
            square,
            square,
            square,
            pltpu.VMEM((F, F), BF16),
            pltpu.VMEM((1, F), F32),
            nodes,
            letters(32),
        ),
        copies=4 * count + 8,
        flops=3 * wide,
        name="first_layer",
    )
    (partial_two,) = call(
        second_terms,
        "hhhhv",
        (shaped(ROWS, F, dtype=F32),),
        (answers, local, edge, hidden),
        own=(peers, square, square, nodes),
        copies=5,
        flops=2 * wide,
        name="second_terms",
    )
    pushed = exchange(push)
    aggregate, term = call(
        second_layer,
        "hhhhhv",
        (shaped(ROWS, F), shaped(F, F, dtype=F32)),
        (pushed, partial_two, gather, cotangent),
        own=(peers, sums, square, nodes, nodes),
        copies=2 * count + 4,
        flops=2 * wide,
        name="second_layer",
    )
    output = jnp.dot(aggregate, w_second, preferred_element_type=F32).astype(BF16)
    return (hidden, output, summed_everywhere(term))


def solution(mesh):
    finer = Mesh(
        mesh.devices.reshape(8, 4, 2, mesh.shape["rep"]), ("dev_0", "dev_1", "dev_2", "rep")
    )
    rows = P(DEV_REP, None)
    return jax.shard_map(
        body,
        mesh=finer,
        in_specs=(rows, rows, rows, P(DEV_REP), rows, rows, rows, P(), P(), P(), rows),
        out_specs=(rows, rows, P()),
        check_vma=False,
    )
```

```python
import jax
import jax.numpy as jnp
from jax import lax
from jax.experimental import pallas as pl
from jax.experimental.pallas import tpu as pltpu
from jax.sharding import Mesh
from jax.sharding import PartitionSpec as P

CHIPS = ("dev_0", "dev_1")
DEV = ("dev_0", "dev_1", "dev_2")
DEV_REP = ("dev_0", "dev_1", "dev_2", "rep")
PEERS, SLOT, HALF, ROWS, F = 64, 16, 128, 1024, 256
STEP = 512
BANK = {
    "local": slice(0, 1024),
    "edge": slice(1024, 2048),
    "flipped": slice(2048, 3072),
    "gather": slice(3072, 4096),
    "high": slice(4096, 4352),
    "low": slice(4352, 4608),
    "cotangent": slice(4608, 4864),
}
VMEM = 67043328

F32, BF16 = jnp.float32, jnp.bfloat16


def dot(a, b):
    return jnp.dot(a, b, preferred_element_type=F32)


def call(body, kinds, outs, operands, *, own=(), copies=0, flops=0, room=16, alias=None, name=None):
    spaces = {"s": pltpu.SMEM, "v": pltpu.VMEM, "h": pltpu.HBM}
    moved = sum(a.size * a.dtype.itemsize for a in (*operands, *outs))
    arrivals = (pltpu.SemaphoreType.DMA((copies,)),) if copies else ()
    specs = [pl.BlockSpec(memory_space=spaces[k]) for k in kinds]
    return pl.pallas_call(
        body,
        out_shape=outs,
        in_specs=specs[: len(operands)],
        out_specs=tuple(specs[len(operands) :]),
        scratch_shapes=(*own, *arrivals),
        input_output_aliases=alias or {},
        compiler_params=pltpu.CompilerParams(vmem_limit_bytes=VMEM - (room << 20)),
        cost_estimate=pl.CostEstimate(flops=flops, bytes_accessed=moved, transcendentals=0),
        name=name,
    )(*operands)


class Copies:
    def __init__(self, semaphores):
        self.semaphores, self.used = semaphores, 0

    def start(self, source, target):
        copy = pltpu.make_async_copy(source, target, self.semaphores.at[self.used])
        self.used += 1
        copy.start()
        return copy

    def stored(self, source, bank, name):
        return self.start(source, bank.at[:, BANK[name]])


def wait(*copies):
    for copy in copies:
        copy.wait()


def shaped(*dims, dtype=BF16):
    return jax.ShapeDtypeStruct(dims, dtype)


def put(message, at, peers, value):
    count = value.shape[0] // SLOT
    message[peers, at : at + SLOT, :] = value[:, :HALF].reshape(count, SLOT, HALF)
    message[peers, at + SLOT : at + 2 * SLOT, :] = value[:, HALF:].reshape(count, SLOT, HALF)


def steps():
    for at in range(0, ROWS, STEP):
        yield slice(at, at + STEP), slice(at // SLOT, (at + STEP) // SLOT)


def send_clusters(owner, x, h, pulled, message, owners, xs, hs, numbers, packed, sem):
    copies = Copies(sem)
    order = copies.start(owner, owners)
    first = copies.start(x, xs)
    rows_in = copies.start(pulled, numbers)
    second = copies.start(h, hs)
    which = lax.broadcasted_iota(jnp.int32, (8, HALF), 0)
    rows_in.wait()
    for a in range(8):
        line = numbers[a : a + 1, :]
        high = (line // 32).astype(F32)
        low = (line % 32).astype(F32)
        tile = jnp.where(which == 0, high, jnp.where(which == 1, low, 0.0)).astype(BF16)
        for b in range(8):
            packed[a * 8 + b, 64:72, :] = tile
    wait(order, first)
    for j in range(PEERS):
        e = owners[0, j]
        rows = slice(j * SLOT, (j + 1) * SLOT)
        packed[e, 0:16, :] = xs[rows, :HALF]
        packed[e, 16:32, :] = xs[rows, HALF:]
    out_x = copies.start(packed.at[:, 0:32, :], message.at[:, 0:32, :])
    second.wait()
    for j in range(PEERS):
        e = owners[0, j]
        rows = slice(j * SLOT, (j + 1) * SLOT)
        packed[e, 32:48, :] = hs[rows, :HALF]
        packed[e, 48:64, :] = hs[rows, HALF:]
    out_h = copies.start(packed.at[:, 32:72, :], message.at[:, 32:72, :])
    wait(out_x, out_h)


def requested(me, tile):
    tile = tile.astype(F32)
    numbers = 32.0 * tile[:, 0:1, :] + tile[:, 1:2, :]
    lane = lax.broadcasted_iota(jnp.int32, (PEERS, SLOT, HALF), 2)
    place = lax.broadcasted_iota(jnp.int32, (PEERS, SLOT, HALF), 1)
    mine = lane == (me % 8) * SLOT + place
    return jnp.sum(jnp.where(mine, numbers, 0.0), axis=2, keepdims=True).reshape(ROWS, 1)


def take(message, at, into):
    into[:, :HALF] = message[:, at : at + SLOT, :].reshape(ROWS, HALF)
    into[:, HALF:] = message[:, at + SLOT : at + 2 * SLOT, :].reshape(ROWS, HALF)


def mask_tiles(occupied, local_in, edge_in, cotangent, bank, local, edge, flipped, sem):
    copies = Copies(sem)
    out = [copies.stored(cotangent, bank, "cotangent")]
    tiles = [slice(i * 128, (i + 1) * 128) for i in range(8)]
    for i, rows in enumerate(tiles):
        for j, cols in enumerate(tiles):
            part = local_in[rows, cols]
            local[rows, cols] = jnp.where(occupied[i, j] != 0, part, jnp.zeros_like(part))
    out.append(copies.stored(local, bank, "local"))
    for i, rows in enumerate(tiles):
        for j, cols in enumerate(tiles):
            part = edge_in[rows, cols]
            part = jnp.where(occupied[i, 8 + j] != 0, part, jnp.zeros_like(part))
            edge[rows, cols] = part
            flipped[cols, rows] = part.T
    out += [copies.stored(edge, bank, "edge"), copies.stored(flipped, bank, "flipped")]
    wait(*out)


def serve(me, message, bank, own_x, reply_far, own_h, flipped, reply, sem):
    copies = Copies(sem)
    last = copies.start(bank.at[:, BANK["flipped"]], flipped)
    take(message, 0, own_x)
    take(message, 32, own_h)
    wanted = requested(me[0], message[:, 64:72, :]).astype(jnp.int32)
    for rows, peers in steps():
        column = lax.broadcasted_iota(jnp.int32, (STEP, ROWS), 1)
        select = (column == wanted[rows]).astype(BF16)
        put(reply, 0, peers, dot(select, own_x[...]).astype(BF16))
        put(reply, 64, peers, dot(select, own_h[...]).astype(BF16))
    last.wait()
    out = []
    for rows, peers in steps():
        put(reply, 32, peers, dot(flipped[rows, :], own_x[...]).astype(BF16))
        out.append(copies.start(reply.at[peers], reply_far.at[peers]))
    wait(*out)


def prepare(me, message, own_x, bank, bank_out, local, gather, high, low, sem):
    copies = Copies(sem)
    first = copies.start(bank.at[:, BANK["local"]], local)
    wanted = jnp.broadcast_to(requested(me[0], message[:, 64:72, :]), (ROWS, HALF))
    row = lax.broadcasted_iota(jnp.int32, (ROWS, HALF), 0).astype(F32)
    for a in range(8):
        cols = slice(a * HALF, (a + 1) * HALF)
        gather[:, cols] = (row == wanted[cols].T[0:1, :]).astype(BF16)
    out = [copies.stored(gather, bank_out, "gather")]
    first.wait()
    for rows, peers in steps():
        total = dot(local[rows, :], own_x[...])
        high[rows, :] = total.astype(BF16)
        low[rows, :] = (total - high[rows, :].astype(F32)).astype(BF16)
    out += [copies.stored(high, bank_out, "high"), copies.stored(low, bank_out, "low")]
    wait(*out)


def first_layer(
    message, bank, w, bias, hidden_far, push_far,
    far, pushed, edge, gather, high, low, flipped, hidden, push, sem,
):
    copies = Copies(sem)
    into = {"edge": edge, "gather": gather, "high": high, "low": low}
    arriving = [
        [copies.start(bank.at[rows, BANK[name]], ref.at[rows]) for name, ref in into.items()]
        for rows, peers in steps()
    ]
    last = copies.start(bank.at[:, BANK["flipped"]], flipped)
    take(message, 0, far)
    take(message, 32, pushed)
    for (rows, peers), parts in zip(steps(), arriving):
        wait(*parts)
        total = high[rows, :].astype(F32) + low[rows, :].astype(F32)
        total = total + dot(edge[rows, :], far[...]) + dot(gather[rows, :], pushed[...])
        value = dot(total.astype(BF16), w[...]) + bias[...]
        hidden[rows, :] = jnp.maximum(value, 0.0).astype(BF16)
    out = [copies.start(hidden, hidden_far)]
    last.wait()
    for rows, peers in steps():
        put(push, 0, peers, dot(flipped[rows, :], hidden[...]).astype(BF16))
        out.append(copies.start(push.at[peers], push_far.at[peers]))
    wait(*out)


def second_terms(message, hidden, bank, partial, far, local, edge, sem):
    copies = Copies(sem)
    parts = [
        copies.start(bank.at[:, BANK["local"]], local),
        copies.start(bank.at[:, BANK["edge"]], edge),
    ]
    take(message, 64, far)
    wait(*parts)
    for rows, peers in steps():
        partial[rows, :] = dot(local[rows, :], hidden[...]) + dot(edge[rows, :], far[...])


def second_layer(message, partial, bank, aggregate, gradient, pushed, gather, cotangent, sem):
    copies = Copies(sem)
    arriving = [
        copies.start(bank.at[rows, BANK["gather"]], gather.at[rows]) for rows, peers in steps()
    ]
    last = copies.start(bank.at[:, BANK["cotangent"]], cotangent)
    take(message, 0, pushed)
    for (rows, peers), part in zip(steps(), arriving):
        part.wait()
        total = partial[rows, :] + dot(gather[rows, :], pushed[...])
        aggregate[rows, :] = total.astype(BF16)
    last.wait()
    gradient[...] = lax.dot_general(
        aggregate[...], cotangent[...], (((0,), (0,)), ((), ())), preferred_element_type=F32
    )


def exchange(message):
    return lax.all_to_all(message, DEV, split_axis=0, concat_axis=0, tiled=True)


def swapped(array, axis, mask):
    return lax.ppermute(array, axis, [(i, i ^ mask) for i in range(lax.axis_size(axis))])


def summed_everywhere(term):
    core = lax.axis_index("dev_2")
    halves = term.reshape(2, ROWS // 8, F)
    kept = lax.dynamic_index_in_dim(halves, core, 0, keepdims=False)
    sent = lax.dynamic_index_in_dim(halves, 1 - core, 0, keepdims=False)
    half = kept + swapped(sent, "dev_2", 1)
    tiles = lax.all_to_all(half.reshape(32, 4, F), CHIPS, split_axis=0, concat_axis=0, tiled=True)
    own = jnp.sum(tiles, axis=0)
    own = (own + swapped(own, "rep", 1)) + (swapped(own, "rep", 2) + swapped(own, "rep", 3))
    copies = jnp.broadcast_to(own[None], (32, 4, F))
    mine = lax.all_to_all(copies, CHIPS, split_axis=0, concat_axis=0, tiled=True).reshape(128, F)
    other = swapped(mine, "dev_2", 1)
    first = jnp.where(core == 0, mine, other)
    second = jnp.where(core == 0, other, mine)
    return jnp.concatenate([first, second], axis=0)


def body(
    features,
    history,
    new_owner,
    pull_rows,
    occupancy,
    adj_local,
    adj_boundary,
    w_first,
    bias_first,
    w_second,
    cotangent,
):
    me = lax.axis_index(DEV).astype(jnp.int32).reshape(1)
    wide = 2 * ROWS * ROWS * F
    nodes, square = pltpu.VMEM((ROWS, F), BF16), pltpu.VMEM((ROWS, ROWS), BF16)
    count = ROWS // STEP

    def letters(rows):
        return pltpu.VMEM((PEERS, rows, HALF), BF16)

    (message,) = call(
        send_clusters,
        "hhhhh",
        (shaped(PEERS, 72, HALF),),
        (new_owner, features, history, pull_rows.reshape(8, 128)),
        own=(
            pltpu.SMEM((1, PEERS), jnp.int32),
            nodes,
            nodes,
            pltpu.VMEM((8, 128), jnp.int32),
            letters(72),
        ),
        copies=6,
        flops=ROWS * F,
        room=0,
        name="send_clusters",
    )
    (bank,) = call(
        mask_tiles,
        "svvvh",
        (shaped(ROWS, 4864),),
        (occupancy, adj_local, adj_boundary, cotangent),
        own=(square, square, square),
        copies=4,
        flops=wide,
        name="mask_tiles",
    )
    arrived = exchange(message)
    own_x, reply = call(
        serve,
        "svhvh",
        (shaped(ROWS, F), shaped(PEERS, 96, HALF)),
        (me, arrived, bank),
        own=(nodes, square, letters(96)),
        copies=1 + count,
        flops=3 * wide,
        room=12,
        name="serve",
    )
    (bank,) = call(
        prepare,
        "svvhh",
        (shaped(ROWS, 4864),),
        (me, arrived, own_x, bank),
        own=(square, square, nodes, nodes),
        copies=4,
        flops=wide,
        alias={3: 0},
        name="prepare",
    )
    answers = exchange(reply)
    hidden, push = call(
        first_layer,
        "vhvvhh",
        (shaped(ROWS, F), shaped(PEERS, 32, HALF)),
        (answers, bank, w_first, bias_first.reshape(1, F)),
        own=(nodes, nodes, square, square, nodes, nodes, square, nodes, letters(32)),
        copies=5 * count + 2,
        flops=3 * wide,
        name="first_layer",
    )
    (partial_two,) = call(
        second_terms,
        "vvhv",
        (shaped(ROWS, F, dtype=F32),),
        (answers, hidden, bank),
        own=(nodes, square, square),
        copies=2,
        flops=2 * wide,
        name="second_terms",
    )
    pushed = exchange(push)
    aggregate, term = call(
        second_layer,
        "vvhvv",
        (shaped(ROWS, F), shaped(F, F, dtype=F32)),
        (pushed, partial_two, bank),
        own=(nodes, square, nodes),
        copies=count + 1,
        flops=2 * wide,
        name="second_layer",
    )
    output = jnp.dot(aggregate, w_second, preferred_element_type=F32).astype(BF16)
    return (hidden, output, summed_everywhere(term))


def solution(mesh):
    finer = Mesh(
        mesh.devices.reshape(8, 4, 2, mesh.shape["rep"]), ("dev_0", "dev_1", "dev_2", "rep")
    )
    rows = P(DEV_REP, None)
    return jax.shard_map(
        body,
        mesh=finer,
        in_specs=(rows, rows, rows, P(DEV_REP), rows, rows, rows, P(), P(), P(), rows),
        out_specs=(rows, rows, P()),
        check_vma=False,
    )
```

```python
import jax
import jax.numpy as jnp
from jax import lax
from jax.experimental import pallas as pl
from jax.experimental.pallas import tpu as pltpu
from jax.sharding import Mesh
from jax.sharding import PartitionSpec as P

CHIPS = ("dev_0", "dev_1")
DEV = ("dev_0", "dev_1", "dev_2")
ORDER = ("dev_2", "dev_0", "dev_1")
DEV_REP = ("dev_0", "dev_1", "dev_2", "rep")
PEERS, SLOT, HALF, ROWS, F = 64, 16, 128, 1024, 256
STEP = 512
BANK = {
    "local": slice(0, 1024),
    "edge": slice(1024, 2048),
    "flipped": slice(2048, 3072),
    "high": slice(3072, 3328),
    "low": slice(3328, 3584),
    "cotangent": slice(3584, 3840),
}
WIDTH = 3840
VMEM = 67043328

F32, BF16 = jnp.float32, jnp.bfloat16


def dot(a, b):
    return jnp.dot(a, b, preferred_element_type=F32)


def call(body, kinds, outs, operands, *, own=(), copies=0, flops=0, room=16, alias=None, name=None):
    spaces = {"s": pltpu.SMEM, "v": pltpu.VMEM, "h": pltpu.HBM}
    moved = sum(a.size * a.dtype.itemsize for a in (*operands, *outs))
    arrivals = (pltpu.SemaphoreType.DMA((copies,)),) if copies else ()
    specs = [pl.BlockSpec(memory_space=spaces[k]) for k in kinds]
    return pl.pallas_call(
        body,
        out_shape=outs,
        in_specs=specs[: len(operands)],
        out_specs=tuple(specs[len(operands) :]),
        scratch_shapes=(*own, *arrivals),
        input_output_aliases=alias or {},
        compiler_params=pltpu.CompilerParams(vmem_limit_bytes=VMEM - (room << 20)),
        cost_estimate=pl.CostEstimate(flops=flops, bytes_accessed=moved, transcendentals=0),
        name=name,
    )(*operands)


class Copies:
    def __init__(self, semaphores):
        self.semaphores, self.used = semaphores, 0

    def start(self, source, target):
        copy = pltpu.make_async_copy(source, target, self.semaphores.at[self.used])
        self.used += 1
        copy.start()
        return copy

    def stored(self, source, bank, name):
        return self.start(source, bank.at[:, BANK[name]])


def wait(*copies):
    for copy in copies:
        copy.wait()


def shaped(*dims, dtype=BF16):
    return jax.ShapeDtypeStruct(dims, dtype)


def place(e):
    return (e & 1) * (PEERS // 2) + (e >> 1)


def put(message, at, peers, value):
    count = value.shape[0] // SLOT
    message[peers, at : at + SLOT, :] = value[:, :HALF].reshape(count, SLOT, HALF)
    message[peers, at + SLOT : at + 2 * SLOT, :] = value[:, HALF:].reshape(count, SLOT, HALF)


def put_by_owner(message, at, peers, value):
    for i, e in enumerate(range(peers.start, peers.stop)):
        block = value[i * SLOT : (i + 1) * SLOT]
        message[place(e), at : at + SLOT, :] = block[:, :HALF]
        message[place(e), at + SLOT : at + 2 * SLOT, :] = block[:, HALF:]


def places(peers):
    for core in range(2):
        yield slice(place(peers.start + core), place(peers.stop - 2 + core) + 1)


def steps(step=STEP):
    for at in range(0, ROWS, step):
        yield slice(at, at + step), slice(at // SLOT, (at + step) // SLOT)


def send_clusters(owner, x, h, pulled, message, owners, xs, hs, numbers, packed, sem):
    copies = Copies(sem)
    order = copies.start(owner, owners)
    first = copies.start(x, xs)
    rows_in = copies.start(pulled, numbers)
    second = copies.start(h, hs)
    which = lax.broadcasted_iota(jnp.int32, (8, HALF), 0)
    rows_in.wait()
    for a in range(8):
        line = numbers[a : a + 1, :]
        high = (line // 32).astype(F32)
        low = (line % 32).astype(F32)
        tile = jnp.where(which == 0, high, jnp.where(which == 1, low, 0.0)).astype(BF16)
        for b in range(8):
            packed[place(a * 8 + b), 64:72, :] = tile
    wait(order, first)
    for j in range(PEERS):
        e = place(owners[0, j])
        rows = slice(j * SLOT, (j + 1) * SLOT)
        packed[e, 0:16, :] = xs[rows, :HALF]
        packed[e, 16:32, :] = xs[rows, HALF:]
    out_x = copies.start(packed.at[:, 0:32, :], message.at[:, 0:32, :])
    second.wait()
    for j in range(PEERS):
        e = place(owners[0, j])
        rows = slice(j * SLOT, (j + 1) * SLOT)
        packed[e, 32:48, :] = hs[rows, :HALF]
        packed[e, 48:64, :] = hs[rows, HALF:]
    out_h = copies.start(packed.at[:, 32:72, :], message.at[:, 32:72, :])
    wait(out_x, out_h)


def requested(me, tile):
    tile = tile.astype(F32)
    numbers = 32.0 * tile[:, 0:1, :] + tile[:, 1:2, :]
    lane = lax.broadcasted_iota(jnp.int32, (PEERS, SLOT, HALF), 2)
    place = lax.broadcasted_iota(jnp.int32, (PEERS, SLOT, HALF), 1)
    mine = lane == (me % 8) * SLOT + place
    return jnp.sum(jnp.where(mine, numbers, 0.0), axis=2, keepdims=True).reshape(ROWS, 1)


def take(message, at, into):
    into[:, :HALF] = message[:, at : at + SLOT, :].reshape(ROWS, HALF)
    into[:, HALF:] = message[:, at + SLOT : at + 2 * SLOT, :].reshape(ROWS, HALF)


def take_by_owner(message, at, into):
    for e in range(PEERS):
        rows = slice(e * SLOT, (e + 1) * SLOT)
        into[rows, :HALF] = message[place(e), at : at + SLOT, :]
        into[rows, HALF:] = message[place(e), at + SLOT : at + 2 * SLOT, :]


def collector(numbers, gather, rows):
    row = lax.broadcasted_iota(jnp.int32, (STEP, HALF), 0).astype(F32) + float(rows.start)
    for a in range(8):
        gather[:, a * HALF : (a + 1) * HALF] = (row == numbers[a : a + 1, :]).astype(BF16)


def mask_tiles(occupied, local_in, edge_in, cotangent, bank, local, edge, flipped, sem):
    copies = Copies(sem)
    out = [copies.stored(cotangent, bank, "cotangent")]
    tiles = [slice(i * 128, (i + 1) * 128) for i in range(8)]
    for i, rows in enumerate(tiles):
        for j, cols in enumerate(tiles):
            part = local_in[rows, cols]
            local[rows, cols] = jnp.where(occupied[i, j] != 0, part, jnp.zeros_like(part))
    out.append(copies.stored(local, bank, "local"))
    for i, rows in enumerate(tiles):
        for j, cols in enumerate(tiles):
            part = edge_in[rows, cols]
            part = jnp.where(occupied[i, 8 + j] != 0, part, jnp.zeros_like(part))
            edge[rows, cols] = part
            flipped[cols, rows] = part.T
    out += [copies.stored(edge, bank, "edge"), copies.stored(flipped, bank, "flipped")]
    wait(*out)


def serve(me, message, bank, own_x, reply_far, own_h, flipped, reply, sem):
    copies = Copies(sem)
    arriving = [
        copies.start(bank.at[rows, BANK["flipped"]], flipped.at[rows]) for rows, peers in steps()
    ]
    take_by_owner(message, 0, own_x)
    take_by_owner(message, 32, own_h)
    wanted = requested(me[0], message[:, 64:72, :]).astype(jnp.int32)
    out = []
    for rows, peers in steps():
        column = lax.broadcasted_iota(jnp.int32, (STEP, ROWS), 1)
        select = (column == wanted[rows]).astype(BF16)
        put(reply, 0, peers, dot(select, own_x[...]).astype(BF16))
        put(reply, 32, peers, dot(select, own_h[...]).astype(BF16))
        out.append(copies.start(reply.at[peers, 0:64], reply_far.at[peers, 0:64]))
    wait(*arriving)
    for rows, peers in steps(STEP // 2):
        put_by_owner(reply, 64, peers, dot(flipped[rows, :], own_x[...]).astype(BF16))
        for part in places(peers):
            out.append(copies.start(reply.at[part, 64:96], reply_far.at[part, 64:96]))
    wait(*out)


def prepare(me, message, own_x, bank, bank_out, numbers, local, high, low, sem):
    copies = Copies(sem)
    first = copies.start(bank.at[:, BANK["local"]], local)
    wanted = jnp.broadcast_to(requested(me[0], message[:, 64:72, :]), (ROWS, HALF))
    for a in range(8):
        numbers[a : a + 1, :] = wanted[a * HALF : (a + 1) * HALF].T[0:1, :]
    first.wait()
    for rows, peers in steps():
        total = dot(local[rows, :], own_x[...])
        high[rows, :] = total.astype(BF16)
        low[rows, :] = (total - high[rows, :].astype(F32)).astype(BF16)
    wait(copies.stored(high, bank_out, "high"), copies.stored(low, bank_out, "low"))


def first_layer(
    message, bank, numbers, w, bias, hidden_far, push_far,
    far, pushed, edge, gather, high, low, sums, flipped, hidden, push, sem,
):
    copies = Copies(sem)
    into = {"edge": edge, "high": high, "low": low}
    arriving = [
        [copies.start(bank.at[rows, BANK[name]], ref.at[rows]) for name, ref in into.items()]
        for rows, peers in steps()
    ]
    last = [
        copies.start(bank.at[rows, BANK["flipped"]], flipped.at[rows]) for rows, peers in steps()
    ]
    take(message, 64, pushed)
    for rows, peers in steps():
        collector(numbers, gather, rows)
        sums[rows, :] = dot(gather[...], pushed[...])
    take_by_owner(message, 0, far)
    for (rows, peers), parts in zip(steps(), arriving):
        wait(*parts)
        total = sums[rows, :] + high[rows, :].astype(F32) + low[rows, :].astype(F32)
        total = total + dot(edge[rows, :], far[...])
        value = dot(total.astype(BF16), w[...]) + bias[...]
        hidden[rows, :] = jnp.maximum(value, 0.0).astype(BF16)
    out = [copies.start(hidden, hidden_far)]
    wait(*last)
    for rows, peers in steps(STEP // 2):
        put_by_owner(push, 0, peers, dot(flipped[rows, :], hidden[...]).astype(BF16))
        for part in places(peers):
            out.append(copies.start(push.at[part], push_far.at[part]))
    wait(*out)


def second_terms(message, hidden, bank, partial, far, local, edge, sem):
    copies = Copies(sem)
    parts = [
        copies.start(bank.at[:, BANK["local"]], local),
        copies.start(bank.at[:, BANK["edge"]], edge),
    ]
    take_by_owner(message, 32, far)
    wait(*parts)
    for rows, peers in steps():
        partial[rows, :] = dot(local[rows, :], hidden[...]) + dot(edge[rows, :], far[...])


def second_layer(message, partial, bank, numbers, aggregate, gradient, pushed, gather, cotangent, sem):
    copies = Copies(sem)
    last = copies.start(bank.at[:, BANK["cotangent"]], cotangent)
    take(message, 0, pushed)
    for rows, peers in steps():
        collector(numbers, gather, rows)
        total = partial[rows, :] + dot(gather[...], pushed[...])
        aggregate[rows, :] = total.astype(BF16)
    last.wait()
    gradient[...] = lax.dot_general(
        aggregate[...], cotangent[...], (((0,), (0,)), ((), ())), preferred_element_type=F32
    )


def exchange(message):
    return lax.all_to_all(message, ORDER, split_axis=0, concat_axis=0, tiled=True)


def swapped(array, axis, mask):
    return lax.ppermute(array, axis, [(i, i ^ mask) for i in range(lax.axis_size(axis))])


def summed_everywhere(term):
    core = lax.axis_index("dev_2")
    halves = term.reshape(2, ROWS // 8, F)
    kept = lax.dynamic_index_in_dim(halves, core, 0, keepdims=False)
    sent = lax.dynamic_index_in_dim(halves, 1 - core, 0, keepdims=False)
    half = kept + swapped(sent, "dev_2", 1)
    tiles = lax.all_to_all(half.reshape(32, 4, F), CHIPS, split_axis=0, concat_axis=0, tiled=True)
    own = jnp.sum(tiles, axis=0)
    own = (own + swapped(own, "rep", 1)) + (swapped(own, "rep", 2) + swapped(own, "rep", 3))
    copies = jnp.broadcast_to(own[None], (32, 4, F))
    mine = lax.all_to_all(copies, CHIPS, split_axis=0, concat_axis=0, tiled=True).reshape(128, F)
    other = swapped(mine, "dev_2", 1)
    first = jnp.where(core == 0, mine, other)
    second = jnp.where(core == 0, other, mine)
    return jnp.concatenate([first, second], axis=0)


def body(
    features,
    history,
    new_owner,
    pull_rows,
    occupancy,
    adj_local,
    adj_boundary,
    w_first,
    bias_first,
    w_second,
    cotangent,
):
    me = lax.axis_index(DEV).astype(jnp.int32).reshape(1)
    wide = 2 * ROWS * ROWS * F
    nodes, square = pltpu.VMEM((ROWS, F), BF16), pltpu.VMEM((ROWS, ROWS), BF16)
    count = ROWS // STEP

    def letters(rows):
        return pltpu.VMEM((PEERS, rows, HALF), BF16)

    (message,) = call(
        send_clusters,
        "hhhhh",
        (shaped(PEERS, 72, HALF),),
        (new_owner, features, history, pull_rows.reshape(8, 128)),
        own=(
            pltpu.SMEM((1, PEERS), jnp.int32),
            nodes,
            nodes,
            pltpu.VMEM((8, 128), jnp.int32),
            letters(72),
        ),
        copies=6,
        flops=ROWS * F,
        room=0,
        name="send_clusters",
    )
    (bank,) = call(
        mask_tiles,
        "svvvh",
        (shaped(ROWS, WIDTH),),
        (occupancy, adj_local, adj_boundary, cotangent),
        own=(square, square, square),
        copies=4,
        flops=wide,
        name="mask_tiles",
    )
    arrived = exchange(message)
    half = pltpu.VMEM((STEP, ROWS), BF16)
    own_x, reply = call(
        serve,
        "svhvh",
        (shaped(ROWS, F), shaped(PEERS, 96, HALF)),
        (me, arrived, bank),
        own=(nodes, square, letters(96)),
        copies=6 * count,
        flops=3 * wide,
        room=12,
        name="serve",
    )
    bank, numbers = call(
        prepare,
        "svvhhv",
        (shaped(ROWS, WIDTH), shaped(8, HALF, dtype=F32)),
        (me, arrived, own_x, bank),
        own=(square, nodes, nodes),
        copies=3,
        flops=wide,
        alias={3: 0},
        name="prepare",
    )
    answers = exchange(reply)
    hidden, push = call(
        first_layer,
        "vhvvvhh",
        (shaped(ROWS, F), shaped(PEERS, 32, HALF)),
        (answers, bank, numbers, w_first, bias_first.reshape(1, F)),
        own=(
            nodes,
            nodes,
            square,
            half,
            nodes,
            nodes,
            pltpu.VMEM((ROWS, F), F32),
            square,
            nodes,
            letters(32),
        ),
        copies=8 * count + 1,
        flops=3 * wide,
        name="first_layer",
    )
    (partial_two,) = call(
        second_terms,
        "vvhv",
        (shaped(ROWS, F, dtype=F32),),
        (answers, hidden, bank),
        own=(nodes, square, square),
        copies=2,
        flops=2 * wide,
        name="second_terms",
    )
    pushed = exchange(push)
    aggregate, term = call(
        second_layer,
        "vvhvvv",
        (shaped(ROWS, F), shaped(F, F, dtype=F32)),
        (pushed, partial_two, bank, numbers),
        own=(nodes, half, nodes),
        copies=1,
        flops=2 * wide,
        name="second_layer",
    )
    output = jnp.dot(aggregate, w_second, preferred_element_type=F32).astype(BF16)
    return (hidden, output, summed_everywhere(term))


def solution(mesh):
    finer = Mesh(
        mesh.devices.reshape(8, 4, 2, mesh.shape["rep"]), ("dev_0", "dev_1", "dev_2", "rep")
    )
    rows = P(DEV_REP, None)
    return jax.shard_map(
        body,
        mesh=finer,
        in_specs=(rows, rows, rows, P(DEV_REP), rows, rows, rows, P(), P(), P(), rows),
        out_specs=(rows, rows, P()),
        check_vma=False,
    )
```

```python
import jax
import jax.numpy as jnp
from jax import lax
from jax.experimental import pallas as pl
from jax.experimental.pallas import tpu as pltpu
from jax.sharding import Mesh
from jax.sharding import PartitionSpec as P

CHIPS = ("dev_0", "dev_1")
DEV = ("dev_0", "dev_1", "dev_2")
ORDER = ("dev_2", "dev_0", "dev_1")
DEV_REP = ("dev_0", "dev_1", "dev_2", "rep")
PEERS, SLOT, HALF, ROWS, F = 64, 16, 128, 1024, 256
STEP = 512
BANK = {
    "local": (0, slice(0, 1024)),
    "edge": (1024, slice(0, 1024)),
    "flipped": (2048, slice(0, 1024)),
    "high": (3072, slice(0, 256)),
    "low": (3072, slice(256, 512)),
    "cotangent": (3072, slice(512, 768)),
}
DEPTH = 4096
VMEM = 67043328

F32, BF16 = jnp.float32, jnp.bfloat16


def dot(a, b):
    return jnp.dot(a, b, preferred_element_type=F32)


def call(body, kinds, outs, operands, *, own=(), copies=0, flops=0, room=16, alias=None, name=None):
    spaces = {"s": pltpu.SMEM, "v": pltpu.VMEM, "h": pltpu.HBM}
    moved = sum(a.size * a.dtype.itemsize for a in (*operands, *outs))
    arrivals = (pltpu.SemaphoreType.DMA((copies,)),) if copies else ()
    specs = [pl.BlockSpec(memory_space=spaces[k]) for k in kinds]
    return pl.pallas_call(
        body,
        out_shape=outs,
        in_specs=specs[: len(operands)],
        out_specs=tuple(specs[len(operands) :]),
        scratch_shapes=(*own, *arrivals),
        input_output_aliases=alias or {},
        compiler_params=pltpu.CompilerParams(vmem_limit_bytes=VMEM - (room << 20)),
        cost_estimate=pl.CostEstimate(flops=flops, bytes_accessed=moved, transcendentals=0),
        name=name,
    )(*operands)


class Copies:
    def __init__(self, semaphores):
        self.semaphores, self.used = semaphores, 0

    def start(self, source, target):
        copy = pltpu.make_async_copy(source, target, self.semaphores.at[self.used])
        self.used += 1
        copy.start()
        return copy

    def stored(self, source, bank, name):
        return self.start(source, kept(bank, name, slice(0, ROWS)))


def kept(bank, name, rows):
    first, columns = BANK[name]
    return bank.at[first + rows.start : first + rows.stop, columns]


def wait(*copies):
    for copy in copies:
        copy.wait()


def shaped(*dims, dtype=BF16):
    return jax.ShapeDtypeStruct(dims, dtype)


def place(e):
    return (e & 1) * (PEERS // 2) + (e >> 1)


def put(message, at, peers, value):
    count = value.shape[0] // SLOT
    message[peers, at : at + SLOT, :] = value[:, :HALF].reshape(count, SLOT, HALF)
    message[peers, at + SLOT : at + 2 * SLOT, :] = value[:, HALF:].reshape(count, SLOT, HALF)


def put_by_owner(message, at, peers, value):
    for i, e in enumerate(range(peers.start, peers.stop)):
        block = value[i * SLOT : (i + 1) * SLOT]
        message[place(e), at : at + SLOT, :] = block[:, :HALF]
        message[place(e), at + SLOT : at + 2 * SLOT, :] = block[:, HALF:]


def places(peers):
    for core in range(2):
        yield slice(place(peers.start + core), place(peers.stop - 2 + core) + 1)


def steps(step=STEP):
    for at in range(0, ROWS, step):
        yield slice(at, at + step), slice(at // SLOT, (at + step) // SLOT)


def send_clusters(owner, x, h, pulled, message, owners, xs, hs, numbers, packed, sem):
    copies = Copies(sem)
    order = copies.start(owner, owners)
    first = copies.start(x, xs)
    rows_in = copies.start(pulled, numbers)
    second = copies.start(h, hs)
    which = lax.broadcasted_iota(jnp.int32, (8, HALF), 0)
    rows_in.wait()
    for a in range(8):
        line = numbers[a : a + 1, :]
        high = (line // 32).astype(F32)
        low = (line % 32).astype(F32)
        tile = jnp.where(which == 0, high, jnp.where(which == 1, low, 0.0)).astype(BF16)
        for b in range(8):
            packed[place(a * 8 + b), 64:72, :] = tile
    wait(order, first)
    for j in range(PEERS):
        e = place(owners[0, j])
        rows = slice(j * SLOT, (j + 1) * SLOT)
        packed[e, 0:16, :] = xs[rows, :HALF]
        packed[e, 16:32, :] = xs[rows, HALF:]
    out_x = copies.start(packed.at[:, 0:32, :], message.at[:, 0:32, :])
    second.wait()
    for j in range(PEERS):
        e = place(owners[0, j])
        rows = slice(j * SLOT, (j + 1) * SLOT)
        packed[e, 32:48, :] = hs[rows, :HALF]
        packed[e, 48:64, :] = hs[rows, HALF:]
    out_h = copies.start(packed.at[:, 32:72, :], message.at[:, 32:72, :])
    wait(out_x, out_h)


def requested(me, tile):
    tile = tile.astype(F32)
    numbers = 32.0 * tile[:, 0:1, :] + tile[:, 1:2, :]
    lane = lax.broadcasted_iota(jnp.int32, (PEERS, SLOT, HALF), 2)
    place = lax.broadcasted_iota(jnp.int32, (PEERS, SLOT, HALF), 1)
    mine = lane == (me % 8) * SLOT + place
    return jnp.sum(jnp.where(mine, numbers, 0.0), axis=2, keepdims=True).reshape(ROWS, 1)


def take(message, at, into):
    into[:, :HALF] = message[:, at : at + SLOT, :].reshape(ROWS, HALF)
    into[:, HALF:] = message[:, at + SLOT : at + 2 * SLOT, :].reshape(ROWS, HALF)


def take_by_owner(message, at, into):
    for e in range(PEERS):
        rows = slice(e * SLOT, (e + 1) * SLOT)
        into[rows, :HALF] = message[place(e), at : at + SLOT, :]
        into[rows, HALF:] = message[place(e), at + SLOT : at + 2 * SLOT, :]


def collector(numbers, gather, rows):
    row = lax.broadcasted_iota(jnp.int32, (STEP, HALF), 0).astype(F32) + float(rows.start)
    for a in range(8):
        gather[:, a * HALF : (a + 1) * HALF] = (row == numbers[a : a + 1, :]).astype(BF16)


def mask_tiles(occupied, local_in, edge_in, cotangent, bank, local, edge, flipped, sem):
    copies = Copies(sem)
    out = [copies.stored(cotangent, bank, "cotangent")]
    tiles = [slice(i * 128, (i + 1) * 128) for i in range(8)]
    for i, rows in enumerate(tiles):
        for j, cols in enumerate(tiles):
            part = local_in[rows, cols]
            local[rows, cols] = jnp.where(occupied[i, j] != 0, part, jnp.zeros_like(part))
    out.append(copies.stored(local, bank, "local"))
    for i, rows in enumerate(tiles):
        for j, cols in enumerate(tiles):
            part = edge_in[rows, cols]
            part = jnp.where(occupied[i, 8 + j] != 0, part, jnp.zeros_like(part))
            edge[rows, cols] = part
            flipped[cols, rows] = part.T
    out += [copies.stored(edge, bank, "edge"), copies.stored(flipped, bank, "flipped")]
    wait(*out)


def serve(me, message, bank, own_x, reply_far, own_h, flipped, reply, sem):
    copies = Copies(sem)
    arriving = [
        copies.start(kept(bank, "flipped", rows), flipped.at[rows]) for rows, peers in steps()
    ]
    take_by_owner(message, 0, own_x)
    take_by_owner(message, 32, own_h)
    wanted = requested(me[0], message[:, 64:72, :]).astype(jnp.int32)
    out = []
    for rows, peers in steps():
        column = lax.broadcasted_iota(jnp.int32, (STEP, ROWS), 1)
        select = (column == wanted[rows]).astype(BF16)
        put(reply, 0, peers, dot(select, own_x[...]).astype(BF16))
        put(reply, 32, peers, dot(select, own_h[...]).astype(BF16))
        out.append(copies.start(reply.at[peers, 0:64], reply_far.at[peers, 0:64]))
    wait(*arriving)
    for rows, peers in steps(STEP // 2):
        put_by_owner(reply, 64, peers, dot(flipped[rows, :], own_x[...]).astype(BF16))
        for part in places(peers):
            out.append(copies.start(reply.at[part, 64:96], reply_far.at[part, 64:96]))
    wait(*out)


def prepare(me, message, own_x, bank, bank_out, numbers, local, high, low, sem):
    copies = Copies(sem)
    first = copies.start(kept(bank, "local", slice(0, ROWS)), local)
    wanted = jnp.broadcast_to(requested(me[0], message[:, 64:72, :]), (ROWS, HALF))
    for a in range(8):
        numbers[a : a + 1, :] = wanted[a * HALF : (a + 1) * HALF].T[0:1, :]
    first.wait()
    for rows, peers in steps():
        total = dot(local[rows, :], own_x[...])
        high[rows, :] = total.astype(BF16)
        low[rows, :] = (total - high[rows, :].astype(F32)).astype(BF16)
    wait(copies.stored(high, bank_out, "high"), copies.stored(low, bank_out, "low"))


def first_layer(
    message, bank, numbers, w, bias, hidden_far, push_far,
    far, pushed, edge, gather, high, low, sums, flipped, hidden, push, sem,
):
    copies = Copies(sem)
    into = {"edge": edge, "high": high, "low": low}
    arriving = [
        [copies.start(kept(bank, name, rows), ref.at[rows]) for name, ref in into.items()]
        for rows, peers in steps()
    ]
    last = [
        copies.start(kept(bank, "flipped", rows), flipped.at[rows]) for rows, peers in steps()
    ]
    take(message, 64, pushed)
    for rows, peers in steps():
        collector(numbers, gather, rows)
        sums[rows, :] = dot(gather[...], pushed[...])
    take_by_owner(message, 0, far)
    for (rows, peers), parts in zip(steps(), arriving):
        wait(*parts)
        total = sums[rows, :] + high[rows, :].astype(F32) + low[rows, :].astype(F32)
        total = total + dot(edge[rows, :], far[...])
        value = dot(total.astype(BF16), w[...]) + bias[...]
        hidden[rows, :] = jnp.maximum(value, 0.0).astype(BF16)
    out = [copies.start(hidden, hidden_far)]
    wait(*last)
    for rows, peers in steps(STEP // 2):
        put_by_owner(push, 0, peers, dot(flipped[rows, :], hidden[...]).astype(BF16))
        for part in places(peers):
            out.append(copies.start(push.at[part], push_far.at[part]))
    wait(*out)


def second_terms(message, hidden, bank, partial, far, local, edge, sem):
    copies = Copies(sem)
    parts = [
        copies.start(kept(bank, "local", slice(0, ROWS)), local),
        copies.start(kept(bank, "edge", slice(0, ROWS)), edge),
    ]
    take_by_owner(message, 32, far)
    wait(*parts)
    for rows, peers in steps():
        partial[rows, :] = dot(local[rows, :], hidden[...]) + dot(edge[rows, :], far[...])


def second_layer(message, partial, bank, numbers, aggregate, gradient, pushed, gather, cotangent, sem):
    copies = Copies(sem)
    last = copies.start(kept(bank, "cotangent", slice(0, ROWS)), cotangent)
    take(message, 0, pushed)
    for rows, peers in steps():
        collector(numbers, gather, rows)
        total = partial[rows, :] + dot(gather[...], pushed[...])
        aggregate[rows, :] = total.astype(BF16)
    last.wait()
    gradient[...] = lax.dot_general(
        aggregate[...], cotangent[...], (((0,), (0,)), ((), ())), preferred_element_type=F32
    )


def exchange(message):
    return lax.all_to_all(message, ORDER, split_axis=0, concat_axis=0, tiled=True)


def swapped(array, axis, mask):
    return lax.ppermute(array, axis, [(i, i ^ mask) for i in range(lax.axis_size(axis))])


def summed_everywhere(term):
    core = lax.axis_index("dev_2")
    halves = term.reshape(2, ROWS // 8, F)
    kept_half = lax.dynamic_index_in_dim(halves, core, 0, keepdims=False)
    sent = lax.dynamic_index_in_dim(halves, 1 - core, 0, keepdims=False)
    half = (kept_half + swapped(sent, "dev_2", 1)).astype(BF16)
    tiles = lax.all_to_all(half.reshape(32, 4, F), CHIPS, split_axis=0, concat_axis=0, tiled=True)
    own = jnp.sum(tiles.astype(F32), axis=0)
    own = (own + swapped(own, "rep", 1)) + (swapped(own, "rep", 2) + swapped(own, "rep", 3))
    copies = jnp.broadcast_to(own.astype(BF16)[None], (32, 4, F))
    mine = lax.all_to_all(copies, CHIPS, split_axis=0, concat_axis=0, tiled=True).reshape(128, F)
    other = swapped(mine, "dev_2", 1)
    first = jnp.where(core == 0, mine, other)
    second = jnp.where(core == 0, other, mine)
    return jnp.concatenate([first, second], axis=0).astype(F32)


def body(
    features,
    history,
    new_owner,
    pull_rows,
    occupancy,
    adj_local,
    adj_boundary,
    w_first,
    bias_first,
    w_second,
    cotangent,
):
    me = lax.axis_index(DEV).astype(jnp.int32).reshape(1)
    wide = 2 * ROWS * ROWS * F
    nodes, square = pltpu.VMEM((ROWS, F), BF16), pltpu.VMEM((ROWS, ROWS), BF16)
    count = ROWS // STEP

    def letters(rows):
        return pltpu.VMEM((PEERS, rows, HALF), BF16)

    (message,) = call(
        send_clusters,
        "hhhhh",
        (shaped(PEERS, 72, HALF),),
        (new_owner, features, history, pull_rows.reshape(8, 128)),
        own=(
            pltpu.SMEM((1, PEERS), jnp.int32),
            nodes,
            nodes,
            pltpu.VMEM((8, 128), jnp.int32),
            letters(72),
        ),
        copies=6,
        flops=ROWS * F,
        room=0,
        name="send_clusters",
    )
    (bank,) = call(
        mask_tiles,
        "svvvh",
        (shaped(DEPTH, ROWS),),
        (occupancy, adj_local, adj_boundary, cotangent),
        own=(square, square, square),
        copies=4,
        flops=wide,
        name="mask_tiles",
    )
    arrived = exchange(message)
    half = pltpu.VMEM((STEP, ROWS), BF16)
    own_x, reply = call(
        serve,
        "svhvh",
        (shaped(ROWS, F), shaped(PEERS, 96, HALF)),
        (me, arrived, bank),
        own=(nodes, square, letters(96)),
        copies=6 * count,
        flops=3 * wide,
        room=12,
        name="serve",
    )
    bank, numbers = call(
        prepare,
        "svvhhv",
        (shaped(DEPTH, ROWS), shaped(8, HALF, dtype=F32)),
        (me, arrived, own_x, bank),
        own=(square, nodes, nodes),
        copies=3,
        flops=wide,
        alias={3: 0},
        name="prepare",
    )
    answers = exchange(reply)
    hidden, push = call(
        first_layer,
        "vhvvvhh",
        (shaped(ROWS, F), shaped(PEERS, 32, HALF)),
        (answers, bank, numbers, w_first, bias_first.reshape(1, F)),
        own=(
            nodes,
            nodes,
            square,
            half,
            nodes,
            nodes,
            pltpu.VMEM((ROWS, F), F32),
            square,
            nodes,
            letters(32),
        ),
        copies=8 * count + 1,
        flops=3 * wide,
        name="first_layer",
    )
    (partial_two,) = call(
        second_terms,
        "vvhv",
        (shaped(ROWS, F, dtype=F32),),
        (answers, hidden, bank),
        own=(nodes, square, square),
        copies=2,
        flops=2 * wide,
        name="second_terms",
    )
    pushed = exchange(push)
    aggregate, term = call(
        second_layer,
        "vvhvvv",
        (shaped(ROWS, F), shaped(F, F, dtype=F32)),
        (pushed, partial_two, bank, numbers),
        own=(nodes, half, nodes),
        copies=1,
        flops=2 * wide,
        name="second_layer",
    )
    output = jnp.dot(aggregate, w_second, preferred_element_type=F32).astype(BF16)
    return (hidden, output, summed_everywhere(term))


def solution(mesh):
    finer = Mesh(
        mesh.devices.reshape(8, 4, 2, mesh.shape["rep"]), ("dev_0", "dev_1", "dev_2", "rep")
    )
    rows = P(DEV_REP, None)
    return jax.shard_map(
        body,
        mesh=finer,
        in_specs=(rows, rows, rows, P(DEV_REP), rows, rows, rows, P(), P(), P(), rows),
        out_specs=(rows, rows, P()),
        check_vma=False,
    )
```

```python
import jax
import jax.numpy as jnp
from jax import lax
from jax.experimental import pallas as pl
from jax.experimental.pallas import tpu as pltpu
from jax.sharding import Mesh
from jax.sharding import PartitionSpec as P

CHIPS = ("dev_0", "dev_1")
DEV = ("dev_0", "dev_1", "dev_2")
ORDER = ("dev_2", "dev_0", "dev_1")
DEV_REP = ("dev_0", "dev_1", "dev_2", "rep")
PEERS, SLOT, HALF, ROWS, F = 64, 16, 128, 1024, 256
STEP = 512
BANK = {
    "local": (0, slice(0, 1024)),
    "edge": (1024, slice(0, 1024)),
    "flipped": (2048, slice(0, 1024)),
    "high": (3072, slice(0, 256)),
    "low": (3072, slice(256, 512)),
    "cotangent": (3072, slice(512, 768)),
}
DEPTH = 4096
VMEM = 67043328

F32, BF16 = jnp.float32, jnp.bfloat16


def dot(a, b):
    return jnp.dot(a, b, preferred_element_type=F32)


def call(body, kinds, outs, operands, *, own=(), copies=0, flops=0, room=16, alias=None, name=None):
    spaces = {"s": pltpu.SMEM, "v": pltpu.VMEM, "h": pltpu.HBM}
    moved = sum(a.size * a.dtype.itemsize for a in (*operands, *outs))
    arrivals = (pltpu.SemaphoreType.DMA((copies,)),) if copies else ()
    specs = [pl.BlockSpec(memory_space=spaces[k]) for k in kinds]
    return pl.pallas_call(
        body,
        out_shape=outs,
        in_specs=specs[: len(operands)],
        out_specs=tuple(specs[len(operands) :]),
        scratch_shapes=(*own, *arrivals),
        input_output_aliases=alias or {},
        compiler_params=pltpu.CompilerParams(vmem_limit_bytes=VMEM - (room << 20)),
        cost_estimate=pl.CostEstimate(flops=flops, bytes_accessed=moved, transcendentals=0),
        name=name,
    )(*operands)


class Copies:
    def __init__(self, semaphores):
        self.semaphores, self.used = semaphores, 0

    def start(self, source, target):
        copy = pltpu.make_async_copy(source, target, self.semaphores.at[self.used])
        self.used += 1
        copy.start()
        return copy

    def stored(self, source, bank, name):
        return self.start(source, kept(bank, name, slice(0, ROWS)))


def kept(bank, name, rows):
    first, columns = BANK[name]
    return bank.at[first + rows.start : first + rows.stop, columns]


def wait(*copies):
    for copy in copies:
        copy.wait()


def dot_flipped(a, b):
    return lax.dot_general(a, b, (((0,), (0,)), ((), ())), preferred_element_type=F32)


def shaped(*dims, dtype=BF16):
    return jax.ShapeDtypeStruct(dims, dtype)


def place(e):
    return (e & 1) * (PEERS // 2) + (e >> 1)


def put(message, at, peers, value):
    count = value.shape[0] // SLOT
    message[peers, at : at + SLOT, :] = value[:, :HALF].reshape(count, SLOT, HALF)
    message[peers, at + SLOT : at + 2 * SLOT, :] = value[:, HALF:].reshape(count, SLOT, HALF)


def put_by_owner(message, at, peers, value):
    for i, e in enumerate(range(peers.start, peers.stop)):
        block = value[i * SLOT : (i + 1) * SLOT]
        message[place(e), at : at + SLOT, :] = block[:, :HALF]
        message[place(e), at + SLOT : at + 2 * SLOT, :] = block[:, HALF:]


def places(peers):
    for core in range(2):
        yield slice(place(peers.start + core), place(peers.stop - 2 + core) + 1)


def steps(step=STEP):
    for at in range(0, ROWS, step):
        yield slice(at, at + step), slice(at // SLOT, (at + step) // SLOT)


def send_clusters(owner, x, h, pulled, message, owners, xs, hs, numbers, packed, sem):
    copies = Copies(sem)
    order = copies.start(owner, owners)
    first = copies.start(x, xs)
    rows_in = copies.start(pulled, numbers)
    second = copies.start(h, hs)
    which = lax.broadcasted_iota(jnp.int32, (8, HALF), 0)
    rows_in.wait()
    for a in range(8):
        line = numbers[a : a + 1, :]
        high = (line // 32).astype(F32)
        low = (line % 32).astype(F32)
        tile = jnp.where(which == 0, high, jnp.where(which == 1, low, 0.0)).astype(BF16)
        for b in range(8):
            packed[place(a * 8 + b), 64:72, :] = tile
    wait(order, first)
    for j in range(PEERS):
        e = place(owners[0, j])
        rows = slice(j * SLOT, (j + 1) * SLOT)
        packed[e, 0:16, :] = xs[rows, :HALF]
        packed[e, 16:32, :] = xs[rows, HALF:]
    out_x = copies.start(packed.at[:, 0:32, :], message.at[:, 0:32, :])
    second.wait()
    for j in range(PEERS):
        e = place(owners[0, j])
        rows = slice(j * SLOT, (j + 1) * SLOT)
        packed[e, 32:48, :] = hs[rows, :HALF]
        packed[e, 48:64, :] = hs[rows, HALF:]
    out_h = copies.start(packed.at[:, 32:72, :], message.at[:, 32:72, :])
    wait(out_x, out_h)


def requested(me, tile):
    tile = tile.astype(F32)
    numbers = 32.0 * tile[:, 0:1, :] + tile[:, 1:2, :]
    lane = lax.broadcasted_iota(jnp.int32, (PEERS, SLOT, HALF), 2)
    place = lax.broadcasted_iota(jnp.int32, (PEERS, SLOT, HALF), 1)
    mine = lane == (me % 8) * SLOT + place
    return jnp.sum(jnp.where(mine, numbers, 0.0), axis=2, keepdims=True).reshape(ROWS, 1)


def take(message, at, into):
    into[:, :HALF] = message[:, at : at + SLOT, :].reshape(ROWS, HALF)
    into[:, HALF:] = message[:, at + SLOT : at + 2 * SLOT, :].reshape(ROWS, HALF)


def take_by_owner(message, at, into):
    for e in range(PEERS):
        rows = slice(e * SLOT, (e + 1) * SLOT)
        into[rows, :HALF] = message[place(e), at : at + SLOT, :]
        into[rows, HALF:] = message[place(e), at + SLOT : at + 2 * SLOT, :]


def collector(numbers, gather, rows):
    row = lax.broadcasted_iota(jnp.int32, (STEP, HALF), 0).astype(F32) + float(rows.start)
    for a in range(8):
        gather[:, a * HALF : (a + 1) * HALF] = (row == numbers[a : a + 1, :]).astype(BF16)


def mask_tiles(occupied, local_in, edge_in, cotangent, bank, local, edge, flipped, sem):
    copies = Copies(sem)
    out = [copies.stored(cotangent, bank, "cotangent")]
    tiles = [slice(i * 128, (i + 1) * 128) for i in range(8)]
    for i, rows in enumerate(tiles):
        for j, cols in enumerate(tiles):
            part = local_in[rows, cols]
            local[rows, cols] = jnp.where(occupied[i, j] != 0, part, jnp.zeros_like(part))
    out.append(copies.stored(local, bank, "local"))
    for i, rows in enumerate(tiles):
        for j, cols in enumerate(tiles):
            part = edge_in[rows, cols]
            part = jnp.where(occupied[i, 8 + j] != 0, part, jnp.zeros_like(part))
            edge[rows, cols] = part
            flipped[cols, rows] = part.T
    out += [copies.stored(edge, bank, "edge"), copies.stored(flipped, bank, "flipped")]
    wait(*out)


def serve(me, message, bank, own_x, reply_far, own_h, flipped, reply, sem):
    copies = Copies(sem)
    arriving = [
        copies.start(kept(bank, "flipped", rows), flipped.at[rows]) for rows, peers in steps()
    ]
    take_by_owner(message, 0, own_x)
    take_by_owner(message, 32, own_h)
    wanted = requested(me[0], message[:, 64:72, :]).astype(jnp.int32)
    out = []
    for rows, peers in steps():
        column = lax.broadcasted_iota(jnp.int32, (STEP, ROWS), 1)
        select = (column == wanted[rows]).astype(BF16)
        put(reply, 0, peers, dot(select, own_x[...]).astype(BF16))
        put(reply, 32, peers, dot(select, own_h[...]).astype(BF16))
        out.append(copies.start(reply.at[peers, 0:64], reply_far.at[peers, 0:64]))
    wait(*arriving)
    for rows, peers in steps(STEP // 2):
        put_by_owner(reply, 64, peers, dot(flipped[rows, :], own_x[...]).astype(BF16))
        for part in places(peers):
            out.append(copies.start(reply.at[part, 64:96], reply_far.at[part, 64:96]))
    wait(*out)


def prepare(me, message, own_x, bank, bank_out, numbers, local, high, low, sem):
    copies = Copies(sem)
    first = copies.start(kept(bank, "local", slice(0, ROWS)), local)
    wanted = jnp.broadcast_to(requested(me[0], message[:, 64:72, :]), (ROWS, HALF))
    for a in range(8):
        numbers[a : a + 1, :] = wanted[a * HALF : (a + 1) * HALF].T[0:1, :]
    first.wait()
    for rows, peers in steps():
        total = dot(local[rows, :], own_x[...])
        high[rows, :] = total.astype(BF16)
        low[rows, :] = (total - high[rows, :].astype(F32)).astype(BF16)
    wait(copies.stored(high, bank_out, "high"), copies.stored(low, bank_out, "low"))


def first_layer(
    message, bank, numbers, w, bias, hidden_far, push_far,
    far, pushed, edge, gather, high, low, sums, hidden, push, sem,
):
    copies = Copies(sem)
    into = {"edge": edge, "high": high, "low": low}
    arriving = [
        [copies.start(kept(bank, name, rows), ref.at[rows]) for name, ref in into.items()]
        for rows, peers in steps()
    ]
    take(message, 64, pushed)
    for rows, peers in steps():
        collector(numbers, gather, rows)
        sums[rows, :] = dot(gather[...], pushed[...])
    take_by_owner(message, 0, far)
    for (rows, peers), parts in zip(steps(), arriving):
        wait(*parts)
        total = sums[rows, :] + high[rows, :].astype(F32) + low[rows, :].astype(F32)
        total = total + dot(edge[rows, :], far[...])
        value = dot(total.astype(BF16), w[...]) + bias[...]
        hidden[rows, :] = jnp.maximum(value, 0.0).astype(BF16)
    out = [copies.start(hidden, hidden_far)]
    for rows, peers in steps(STEP // 2):
        put_by_owner(push, 0, peers, dot_flipped(edge[:, rows], hidden[...]).astype(BF16))
        for part in places(peers):
            out.append(copies.start(push.at[part], push_far.at[part]))
    wait(*out)


def second_terms(message, hidden, bank, partial, far, local, edge, sem):
    copies = Copies(sem)
    parts = [
        copies.start(kept(bank, "local", slice(0, ROWS)), local),
        copies.start(kept(bank, "edge", slice(0, ROWS)), edge),
    ]
    take_by_owner(message, 32, far)
    wait(*parts)
    for rows, peers in steps():
        partial[rows, :] = dot(local[rows, :], hidden[...]) + dot(edge[rows, :], far[...])


def second_layer(message, partial, bank, numbers, aggregate, gradient, pushed, gather, cotangent, sem):
    copies = Copies(sem)
    last = copies.start(kept(bank, "cotangent", slice(0, ROWS)), cotangent)
    take(message, 0, pushed)
    for rows, peers in steps():
        collector(numbers, gather, rows)
        total = partial[rows, :] + dot(gather[...], pushed[...])
        aggregate[rows, :] = total.astype(BF16)
    last.wait()
    gradient[...] = lax.dot_general(
        aggregate[...], cotangent[...], (((0,), (0,)), ((), ())), preferred_element_type=F32
    )


def exchange(message):
    return lax.all_to_all(message, ORDER, split_axis=0, concat_axis=0, tiled=True)


def swapped(array, axis, mask):
    return lax.ppermute(array, axis, [(i, i ^ mask) for i in range(lax.axis_size(axis))])


def summed_everywhere(term):
    core = lax.axis_index("dev_2")
    halves = term.reshape(2, ROWS // 8, F)
    kept_half = lax.dynamic_index_in_dim(halves, core, 0, keepdims=False)
    sent = lax.dynamic_index_in_dim(halves, 1 - core, 0, keepdims=False)
    half = (kept_half + swapped(sent, "dev_2", 1)).astype(BF16)
    tiles = lax.all_to_all(half.reshape(32, 4, F), CHIPS, split_axis=0, concat_axis=0, tiled=True)
    own = jnp.sum(tiles.astype(F32), axis=0)
    own = (own + swapped(own, "rep", 1)) + (swapped(own, "rep", 2) + swapped(own, "rep", 3))
    copies = jnp.broadcast_to(own.astype(BF16)[None], (32, 4, F))
    mine = lax.all_to_all(copies, CHIPS, split_axis=0, concat_axis=0, tiled=True).reshape(128, F)
    other = swapped(mine, "dev_2", 1)
    first = jnp.where(core == 0, mine, other)
    second = jnp.where(core == 0, other, mine)
    return jnp.concatenate([first, second], axis=0).astype(F32)


def body(
    features,
    history,
    new_owner,
    pull_rows,
    occupancy,
    adj_local,
    adj_boundary,
    w_first,
    bias_first,
    w_second,
    cotangent,
):
    me = lax.axis_index(DEV).astype(jnp.int32).reshape(1)
    wide = 2 * ROWS * ROWS * F
    nodes, square = pltpu.VMEM((ROWS, F), BF16), pltpu.VMEM((ROWS, ROWS), BF16)
    count = ROWS // STEP

    def letters(rows):
        return pltpu.VMEM((PEERS, rows, HALF), BF16)

    (message,) = call(
        send_clusters,
        "hhhhh",
        (shaped(PEERS, 72, HALF),),
        (new_owner, features, history, pull_rows.reshape(8, 128)),
        own=(
            pltpu.SMEM((1, PEERS), jnp.int32),
            nodes,
            nodes,
            pltpu.VMEM((8, 128), jnp.int32),
            letters(72),
        ),
        copies=6,
        flops=ROWS * F,
        room=0,
        name="send_clusters",
    )
    (bank,) = call(
        mask_tiles,
        "svvvh",
        (shaped(DEPTH, ROWS),),
        (occupancy, adj_local, adj_boundary, cotangent),
        own=(square, square, square),
        copies=4,
        flops=wide,
        name="mask_tiles",
    )
    arrived = exchange(message)
    half = pltpu.VMEM((STEP, ROWS), BF16)
    own_x, reply = call(
        serve,
        "svhvh",
        (shaped(ROWS, F), shaped(PEERS, 96, HALF)),
        (me, arrived, bank),
        own=(nodes, square, letters(96)),
        copies=6 * count,
        flops=3 * wide,
        room=12,
        name="serve",
    )
    bank, numbers = call(
        prepare,
        "svvhhv",
        (shaped(DEPTH, ROWS), shaped(8, HALF, dtype=F32)),
        (me, arrived, own_x, bank),
        own=(square, nodes, nodes),
        copies=3,
        flops=wide,
        alias={3: 0},
        name="prepare",
    )
    answers = exchange(reply)
    hidden, push = call(
        first_layer,
        "vhvvvhh",
        (shaped(ROWS, F), shaped(PEERS, 32, HALF)),
        (answers, bank, numbers, w_first, bias_first.reshape(1, F)),
        own=(
            nodes,
            nodes,
            square,
            half,
            nodes,
            nodes,
            pltpu.VMEM((ROWS, F), F32),
            nodes,
            letters(32),
        ),
        copies=7 * count + 1,
        flops=3 * wide,
        name="first_layer",
    )
    (partial_two,) = call(
        second_terms,
        "vvhv",
        (shaped(ROWS, F, dtype=F32),),
        (answers, hidden, bank),
        own=(nodes, square, square),
        copies=2,
        flops=2 * wide,
        name="second_terms",
    )
    pushed = exchange(push)
    aggregate, term = call(
        second_layer,
        "vvhvvv",
        (shaped(ROWS, F), shaped(F, F, dtype=F32)),
        (pushed, partial_two, bank, numbers),
        own=(nodes, half, nodes),
        copies=1,
        flops=2 * wide,
        name="second_layer",
    )
    output = jnp.dot(aggregate, w_second, preferred_element_type=F32).astype(BF16)
    return (hidden, output, summed_everywhere(term))


def solution(mesh):
    finer = Mesh(
        mesh.devices.reshape(8, 4, 2, mesh.shape["rep"]), ("dev_0", "dev_1", "dev_2", "rep")
    )
    rows = P(DEV_REP, None)
    return jax.shard_map(
        body,
        mesh=finer,
        in_specs=(rows, rows, rows, P(DEV_REP), rows, rows, rows, P(), P(), P(), rows),
        out_specs=(rows, rows, P()),
        check_vma=False,
    )
```

```python
import jax
import jax.numpy as jnp
from jax import lax
from jax.experimental import pallas as pl
from jax.experimental.pallas import tpu as pltpu
from jax.sharding import Mesh
from jax.sharding import PartitionSpec as P

CHIPS = ("dev_0", "dev_1")
DEV = ("dev_0", "dev_1", "dev_2")
ORDER = ("dev_2", "dev_0", "dev_1")
DEV_REP = ("dev_0", "dev_1", "dev_2", "rep")
PEERS, SLOT, HALF, ROWS, F = 64, 16, 128, 1024, 256
STEP = 512
BANK = {
    "local": (0, slice(0, 1024)),
    "edge": (1024, slice(0, 1024)),
    "flipped": (2048, slice(0, 1024)),
    "high": (3072, slice(0, 256)),
    "low": (3072, slice(256, 512)),
    "cotangent": (3072, slice(512, 768)),
}
DEPTH = 4096
VMEM = 67043328

F32, BF16 = jnp.float32, jnp.bfloat16


def dot(a, b):
    return jnp.dot(a, b, preferred_element_type=F32)


def call(body, kinds, outs, operands, *, own=(), copies=0, flops=0, room=16, alias=None, name=None):
    spaces = {"s": pltpu.SMEM, "v": pltpu.VMEM, "h": pltpu.HBM}
    moved = sum(a.size * a.dtype.itemsize for a in (*operands, *outs))
    arrivals = (pltpu.SemaphoreType.DMA((copies,)),) if copies else ()
    specs = [pl.BlockSpec(memory_space=spaces[k]) for k in kinds]
    return pl.pallas_call(
        body,
        out_shape=outs,
        in_specs=specs[: len(operands)],
        out_specs=tuple(specs[len(operands) :]),
        scratch_shapes=(*own, *arrivals),
        input_output_aliases=alias or {},
        compiler_params=pltpu.CompilerParams(vmem_limit_bytes=VMEM - (room << 20)),
        cost_estimate=pl.CostEstimate(flops=flops, bytes_accessed=moved, transcendentals=0),
        name=name,
    )(*operands)


class Copies:
    def __init__(self, semaphores):
        self.semaphores, self.used = semaphores, 0

    def start(self, source, target):
        copy = pltpu.make_async_copy(source, target, self.semaphores.at[self.used])
        self.used += 1
        copy.start()
        return copy

    def stored(self, source, bank, name):
        return self.start(source, kept(bank, name, slice(0, ROWS)))


def kept(bank, name, rows):
    first, columns = BANK[name]
    return bank.at[first + rows.start : first + rows.stop, columns]


def wait(*copies):
    for copy in copies:
        copy.wait()


def dot_flipped(a, b):
    return lax.dot_general(a, b, (((0,), (0,)), ((), ())), preferred_element_type=F32)


def shaped(*dims, dtype=BF16):
    return jax.ShapeDtypeStruct(dims, dtype)


def place(e):
    return (e & 1) * (PEERS // 2) + (e >> 1)


def put(message, at, peers, value):
    count = value.shape[0] // SLOT
    message[peers, at : at + SLOT, :] = value[:, :HALF].reshape(count, SLOT, HALF)
    message[peers, at + SLOT : at + 2 * SLOT, :] = value[:, HALF:].reshape(count, SLOT, HALF)


def put_by_owner(message, at, peers, value):
    for i, e in enumerate(range(peers.start, peers.stop)):
        block = value[i * SLOT : (i + 1) * SLOT]
        message[place(e), at : at + SLOT, :] = block[:, :HALF]
        message[place(e), at + SLOT : at + 2 * SLOT, :] = block[:, HALF:]


def places(peers):
    for core in range(2):
        yield slice(place(peers.start + core), place(peers.stop - 2 + core) + 1)


def steps(step=STEP):
    for at in range(0, ROWS, step):
        yield slice(at, at + step), slice(at // SLOT, (at + step) // SLOT)


def send_clusters(owner, x, h, pulled, message, owners, xs, hs, numbers, packed, sem):
    copies = Copies(sem)
    order = copies.start(owner, owners)
    first = copies.start(x, xs)
    rows_in = copies.start(pulled, numbers)
    second = copies.start(h, hs)
    which = lax.broadcasted_iota(jnp.int32, (8, HALF), 0)
    rows_in.wait()
    for a in range(8):
        line = numbers[a : a + 1, :]
        high = (line // 32).astype(F32)
        low = (line % 32).astype(F32)
        tile = jnp.where(which == 0, high, jnp.where(which == 1, low, 0.0)).astype(BF16)
        for b in range(8):
            packed[place(a * 8 + b), 64:72, :] = tile
    wait(order, first)
    for j in range(PEERS):
        e = place(owners[0, j])
        rows = slice(j * SLOT, (j + 1) * SLOT)
        packed[e, 0:16, :] = xs[rows, :HALF]
        packed[e, 16:32, :] = xs[rows, HALF:]
    out_x = copies.start(packed.at[:, 0:32, :], message.at[:, 0:32, :])
    second.wait()
    for j in range(PEERS):
        e = place(owners[0, j])
        rows = slice(j * SLOT, (j + 1) * SLOT)
        packed[e, 32:48, :] = hs[rows, :HALF]
        packed[e, 48:64, :] = hs[rows, HALF:]
    out_h = copies.start(packed.at[:, 32:72, :], message.at[:, 32:72, :])
    wait(out_x, out_h)


def requested(me, tile):
    tile = tile.astype(F32)
    numbers = 32.0 * tile[:, 0:1, :] + tile[:, 1:2, :]
    lane = lax.broadcasted_iota(jnp.int32, (PEERS, SLOT, HALF), 2)
    place = lax.broadcasted_iota(jnp.int32, (PEERS, SLOT, HALF), 1)
    mine = lane == (me % 8) * SLOT + place
    return jnp.sum(jnp.where(mine, numbers, 0.0), axis=2, keepdims=True).reshape(ROWS, 1)


def take(message, at, into):
    into[:, :HALF] = message[:, at : at + SLOT, :].reshape(ROWS, HALF)
    into[:, HALF:] = message[:, at + SLOT : at + 2 * SLOT, :].reshape(ROWS, HALF)


def take_by_owner(message, at, into):
    for e in range(PEERS):
        rows = slice(e * SLOT, (e + 1) * SLOT)
        into[rows, :HALF] = message[place(e), at : at + SLOT, :]
        into[rows, HALF:] = message[place(e), at + SLOT : at + 2 * SLOT, :]


def collector(numbers, gather, rows):
    row = lax.broadcasted_iota(jnp.int32, (STEP, HALF), 0).astype(F32) + float(rows.start)
    for a in range(8):
        gather[:, a * HALF : (a + 1) * HALF] = (row == numbers[a : a + 1, :]).astype(BF16)


def mask_tiles(occupied, local_in, edge_in, cotangent, bank, local, edge, flipped, sem):
    copies = Copies(sem)
    out = [copies.stored(cotangent, bank, "cotangent")]
    tiles = [slice(i * 128, (i + 1) * 128) for i in range(8)]
    for i, rows in enumerate(tiles):
        for j, cols in enumerate(tiles):
            part = local_in[rows, cols]
            local[rows, cols] = jnp.where(occupied[i, j] != 0, part, jnp.zeros_like(part))
    out.append(copies.stored(local, bank, "local"))
    for i, rows in enumerate(tiles):
        for j, cols in enumerate(tiles):
            part = edge_in[rows, cols]
            part = jnp.where(occupied[i, 8 + j] != 0, part, jnp.zeros_like(part))
            edge[rows, cols] = part
            flipped[cols, rows] = part.T
    out += [copies.stored(edge, bank, "edge"), copies.stored(flipped, bank, "flipped")]
    wait(*out)


def serve(me, message, bank, own_x, reply_far, own_h, flipped, reply, sem):
    copies = Copies(sem)
    arriving = [
        copies.start(kept(bank, "flipped", rows), flipped.at[rows]) for rows, peers in steps()
    ]
    take_by_owner(message, 0, own_x)
    take_by_owner(message, 32, own_h)
    wanted = requested(me[0], message[:, 64:72, :]).astype(jnp.int32)
    out = []
    for rows, peers in steps():
        column = lax.broadcasted_iota(jnp.int32, (STEP, ROWS), 1)
        select = (column == wanted[rows]).astype(BF16)
        put(reply, 0, peers, dot(select, own_x[...]).astype(BF16))
        put(reply, 32, peers, dot(select, own_h[...]).astype(BF16))
        out.append(copies.start(reply.at[peers, 0:64], reply_far.at[peers, 0:64]))
    wait(*arriving)
    for rows, peers in steps(STEP // 2):
        put_by_owner(reply, 64, peers, dot(flipped[rows, :], own_x[...]).astype(BF16))
        for part in places(peers):
            out.append(copies.start(reply.at[part, 64:96], reply_far.at[part, 64:96]))
    wait(*out)


def prepare(me, message, own_x, bank, bank_out, numbers, local, high, low, sem):
    copies = Copies(sem)
    first = copies.start(kept(bank, "local", slice(0, ROWS)), local)
    wanted = jnp.broadcast_to(requested(me[0], message[:, 64:72, :]), (ROWS, HALF))
    for a in range(8):
        numbers[a : a + 1, :] = wanted[a * HALF : (a + 1) * HALF].T[0:1, :]
    first.wait()
    for rows, peers in steps():
        total = dot(local[rows, :], own_x[...])
        high[rows, :] = total.astype(BF16)
        low[rows, :] = (total - high[rows, :].astype(F32)).astype(BF16)
    wait(copies.stored(high, bank_out, "high"), copies.stored(low, bank_out, "low"))


def first_layer(
    message, bank, numbers, w, bias, hidden_far, push_far,
    far, pushed, edge, gather, high, low, sums, hidden, push, sem,
):
    copies = Copies(sem)
    into = {"edge": edge, "high": high, "low": low}
    arriving = [
        [copies.start(kept(bank, name, rows), ref.at[rows]) for name, ref in into.items()]
        for rows, peers in steps()
    ]
    take(message, 64, pushed)
    for rows, peers in steps():
        collector(numbers, gather, rows)
        sums[rows, :] = dot(gather[...], pushed[...])
    take_by_owner(message, 0, far)
    for (rows, peers), parts in zip(steps(), arriving):
        wait(*parts)
        total = sums[rows, :] + high[rows, :].astype(F32) + low[rows, :].astype(F32)
        total = total + dot(edge[rows, :], far[...])
        value = dot(total.astype(BF16), w[...]) + bias[...]
        hidden[rows, :] = jnp.maximum(value, 0.0).astype(BF16)
    out = [copies.start(hidden, hidden_far)]
    for rows, peers in steps(STEP // 2):
        put_by_owner(push, 0, peers, dot_flipped(edge[:, rows], hidden[...]).astype(BF16))
        for part in places(peers):
            out.append(copies.start(push.at[part], push_far.at[part]))
    wait(*out)


def second_terms(message, hidden, bank, partial, far, local, edge, sem):
    copies = Copies(sem)
    parts = [
        copies.start(kept(bank, "local", slice(0, ROWS)), local),
        copies.start(kept(bank, "edge", slice(0, ROWS)), edge),
    ]
    take_by_owner(message, 32, far)
    wait(*parts)
    for rows, peers in steps():
        partial[rows, :] = dot(local[rows, :], hidden[...]) + dot(edge[rows, :], far[...])


def second_layer(message, partial, bank, numbers, aggregate, gradient, pushed, gather, cotangent, sem):
    copies = Copies(sem)
    last = copies.start(kept(bank, "cotangent", slice(0, ROWS)), cotangent)
    take(message, 0, pushed)
    for rows, peers in steps():
        collector(numbers, gather, rows)
        total = partial[rows, :] + dot(gather[...], pushed[...])
        aggregate[rows, :] = total.astype(BF16)
    last.wait()
    gradient[...] = lax.dot_general(
        aggregate[...], cotangent[...], (((0,), (0,)), ((), ())), preferred_element_type=F32
    )


def exchange(message):
    return lax.all_to_all(message, ORDER, split_axis=0, concat_axis=0, tiled=True)


def swapped(array, axis, mask):
    return lax.ppermute(array, axis, [(i, i ^ mask) for i in range(lax.axis_size(axis))])


def summed_everywhere(term):
    core = lax.axis_index("dev_2")
    halves = term.reshape(2, ROWS // 8, F)
    kept_half = lax.dynamic_index_in_dim(halves, core, 0, keepdims=False)
    sent = lax.dynamic_index_in_dim(halves, 1 - core, 0, keepdims=False)
    half = (kept_half + swapped(sent, "dev_2", 1)).astype(BF16)
    tiles = lax.all_to_all(half.reshape(32, 4, F), CHIPS, split_axis=0, concat_axis=0, tiled=True)
    own = lax.optimization_barrier(jnp.sum(tiles.astype(F32), axis=0)).astype(BF16)
    copies = jnp.broadcast_to(own[None], (128, 4, F))
    all_terms = lax.all_to_all(copies, (*CHIPS, "rep"), split_axis=0, concat_axis=0, tiled=True)
    mine = jnp.sum(all_terms.reshape(32, 4, 4, F).astype(F32), axis=1).reshape(128, F)
    other = swapped(mine, "dev_2", 1)
    first = jnp.where(core == 0, mine, other)
    second = jnp.where(core == 0, other, mine)
    return jnp.concatenate([first, second], axis=0)


def body(
    features,
    history,
    new_owner,
    pull_rows,
    occupancy,
    adj_local,
    adj_boundary,
    w_first,
    bias_first,
    w_second,
    cotangent,
):
    me = lax.axis_index(DEV).astype(jnp.int32).reshape(1)
    wide = 2 * ROWS * ROWS * F
    nodes, square = pltpu.VMEM((ROWS, F), BF16), pltpu.VMEM((ROWS, ROWS), BF16)
    count = ROWS // STEP

    def letters(rows):
        return pltpu.VMEM((PEERS, rows, HALF), BF16)

    (message,) = call(
        send_clusters,
        "hhhhh",
        (shaped(PEERS, 72, HALF),),
        (new_owner, features, history, pull_rows.reshape(8, 128)),
        own=(
            pltpu.SMEM((1, PEERS), jnp.int32),
            nodes,
            nodes,
            pltpu.VMEM((8, 128), jnp.int32),
            letters(72),
        ),
        copies=6,
        flops=ROWS * F,
        room=0,
        name="send_clusters",
    )
    (bank,) = call(
        mask_tiles,
        "svvvh",
        (shaped(DEPTH, ROWS),),
        (occupancy, adj_local, adj_boundary, cotangent),
        own=(square, square, square),
        copies=4,
        flops=wide,
        name="mask_tiles",
    )
    arrived = exchange(message)
    half = pltpu.VMEM((STEP, ROWS), BF16)
    own_x, reply = call(
        serve,
        "svhvh",
        (shaped(ROWS, F), shaped(PEERS, 96, HALF)),
        (me, arrived, bank),
        own=(nodes, square, letters(96)),
        copies=6 * count,
        flops=3 * wide,
        room=12,
        name="serve",
    )
    bank, numbers = call(
        prepare,
        "svvhhv",
        (shaped(DEPTH, ROWS), shaped(8, HALF, dtype=F32)),
        (me, arrived, own_x, bank),
        own=(square, nodes, nodes),
        copies=3,
        flops=wide,
        alias={3: 0},
        name="prepare",
    )
    answers = exchange(reply)
    hidden, push = call(
        first_layer,
        "vhvvvhh",
        (shaped(ROWS, F), shaped(PEERS, 32, HALF)),
        (answers, bank, numbers, w_first, bias_first.reshape(1, F)),
        own=(
            nodes,
            nodes,
            square,
            half,
            nodes,
            nodes,
            pltpu.VMEM((ROWS, F), F32),
            nodes,
            letters(32),
        ),
        copies=7 * count + 1,
        flops=3 * wide,
        name="first_layer",
    )
    (partial_two,) = call(
        second_terms,
        "vvhv",
        (shaped(ROWS, F, dtype=F32),),
        (answers, hidden, bank),
        own=(nodes, square, square),
        copies=2,
        flops=2 * wide,
        name="second_terms",
    )
    pushed = exchange(push)
    aggregate, term = call(
        second_layer,
        "vvhvvv",
        (shaped(ROWS, F), shaped(F, F, dtype=F32)),
        (pushed, partial_two, bank, numbers),
        own=(nodes, half, nodes),
        copies=1,
        flops=2 * wide,
        name="second_layer",
    )
    output = jnp.dot(aggregate, w_second, preferred_element_type=F32).astype(BF16)
    return (hidden, output, summed_everywhere(term))


def solution(mesh):
    finer = Mesh(
        mesh.devices.reshape(8, 4, 2, mesh.shape["rep"]), ("dev_0", "dev_1", "dev_2", "rep")
    )
    rows = P(DEV_REP, None)
    return jax.shard_map(
        body,
        mesh=finer,
        in_specs=(rows, rows, rows, P(DEV_REP), rows, rows, rows, P(), P(), P(), rows),
        out_specs=(rows, rows, P()),
        check_vma=False,
    )
```

```python
import jax
import jax.numpy as jnp
from jax import lax
from jax.experimental import pallas as pl
from jax.experimental.pallas import tpu as pltpu
from jax.sharding import Mesh
from jax.sharding import PartitionSpec as P

CHIPS = ("dev_0", "dev_1")
DEV = ("dev_0", "dev_1", "dev_2")
ORDER = ("dev_2", "dev_0", "dev_1")
DEV_REP = ("dev_0", "dev_1", "dev_2", "rep")
PEERS, SLOT, HALF, ROWS, F = 64, 16, 128, 1024, 256
STEP = 512
BANK = {
    "local": (0, slice(0, 1024)),
    "edge": (1024, slice(0, 1024)),
    "flipped": (2048, slice(0, 1024)),
    "high": (3072, slice(0, 256)),
    "low": (3072, slice(256, 512)),
    "cotangent": (3072, slice(512, 768)),
}
DEPTH = 4096
VMEM = 67043328

F32, BF16 = jnp.float32, jnp.bfloat16


def dot(a, b):
    return jnp.dot(a, b, preferred_element_type=F32)


def call(body, kinds, outs, operands, *, own=(), copies=0, flops=0, room=16, alias=None, name=None):
    spaces = {"s": pltpu.SMEM, "v": pltpu.VMEM, "h": pltpu.HBM}
    moved = sum(a.size * a.dtype.itemsize for a in (*operands, *outs))
    arrivals = (pltpu.SemaphoreType.DMA((copies,)),) if copies else ()
    specs = [pl.BlockSpec(memory_space=spaces[k]) for k in kinds]
    return pl.pallas_call(
        body,
        out_shape=outs,
        in_specs=specs[: len(operands)],
        out_specs=tuple(specs[len(operands) :]),
        scratch_shapes=(*own, *arrivals),
        input_output_aliases=alias or {},
        compiler_params=pltpu.CompilerParams(vmem_limit_bytes=VMEM - (room << 20)),
        cost_estimate=pl.CostEstimate(flops=flops, bytes_accessed=moved, transcendentals=0),
        name=name,
    )(*operands)


class Copies:
    def __init__(self, semaphores):
        self.semaphores, self.used = semaphores, 0

    def start(self, source, target):
        copy = pltpu.make_async_copy(source, target, self.semaphores.at[self.used])
        self.used += 1
        copy.start()
        return copy

    def stored(self, source, bank, name):
        return self.start(source, kept(bank, name, slice(0, ROWS)))


def kept(bank, name, rows):
    first, columns = BANK[name]
    return bank.at[first + rows.start : first + rows.stop, columns]


def wait(*copies):
    for copy in copies:
        copy.wait()


def dot_flipped(a, b):
    return lax.dot_general(a, b, (((0,), (0,)), ((), ())), preferred_element_type=F32)


def shaped(*dims, dtype=BF16):
    return jax.ShapeDtypeStruct(dims, dtype)


def place(e):
    return (e & 1) * (PEERS // 2) + (e >> 1)


def put(message, at, peers, value):
    count = value.shape[0] // SLOT
    message[peers, at : at + SLOT, :] = value[:, :HALF].reshape(count, SLOT, HALF)
    message[peers, at + SLOT : at + 2 * SLOT, :] = value[:, HALF:].reshape(count, SLOT, HALF)


def put_by_owner(message, at, peers, value):
    for i, e in enumerate(range(peers.start, peers.stop)):
        block = value[i * SLOT : (i + 1) * SLOT]
        message[place(e), at : at + SLOT, :] = block[:, :HALF]
        message[place(e), at + SLOT : at + 2 * SLOT, :] = block[:, HALF:]


def places(peers):
    for core in range(2):
        yield slice(place(peers.start + core), place(peers.stop - 2 + core) + 1)


def steps(step=STEP):
    for at in range(0, ROWS, step):
        yield slice(at, at + step), slice(at // SLOT, (at + step) // SLOT)


def send_clusters(owner, x, h, pulled, message, owners, xs, hs, numbers, packed, sem):
    copies = Copies(sem)
    order = copies.start(owner, owners)
    first = copies.start(x, xs)
    rows_in = copies.start(pulled, numbers)
    second = copies.start(h, hs)
    which = lax.broadcasted_iota(jnp.int32, (8, HALF), 0)
    rows_in.wait()
    for a in range(8):
        line = numbers[a : a + 1, :]
        high = (line // 32).astype(F32)
        low = (line % 32).astype(F32)
        tile = jnp.where(which == 0, high, jnp.where(which == 1, low, 0.0)).astype(BF16)
        for b in range(8):
            packed[place(a * 8 + b), 64:72, :] = tile
    wait(order, first)
    for j in range(PEERS):
        e = place(owners[0, j])
        rows = slice(j * SLOT, (j + 1) * SLOT)
        packed[e, 0:16, :] = xs[rows, :HALF]
        packed[e, 16:32, :] = xs[rows, HALF:]
    out_x = copies.start(packed.at[:, 0:32, :], message.at[:, 0:32, :])
    second.wait()
    for j in range(PEERS):
        e = place(owners[0, j])
        rows = slice(j * SLOT, (j + 1) * SLOT)
        packed[e, 32:48, :] = hs[rows, :HALF]
        packed[e, 48:64, :] = hs[rows, HALF:]
    out_h = copies.start(packed.at[:, 32:72, :], message.at[:, 32:72, :])
    wait(out_x, out_h)


def requested(me, tile):
    tile = tile.astype(F32)
    numbers = 32.0 * tile[:, 0:1, :] + tile[:, 1:2, :]
    lane = lax.broadcasted_iota(jnp.int32, (PEERS, SLOT, HALF), 2)
    place = lax.broadcasted_iota(jnp.int32, (PEERS, SLOT, HALF), 1)
    mine = lane == (me % 8) * SLOT + place
    return jnp.sum(jnp.where(mine, numbers, 0.0), axis=2, keepdims=True).reshape(ROWS, 1)


def take(message, at, into):
    into[:, :HALF] = message[:, at : at + SLOT, :].reshape(ROWS, HALF)
    into[:, HALF:] = message[:, at + SLOT : at + 2 * SLOT, :].reshape(ROWS, HALF)


def take_by_owner(message, at, into):
    for e in range(PEERS):
        rows = slice(e * SLOT, (e + 1) * SLOT)
        into[rows, :HALF] = message[place(e), at : at + SLOT, :]
        into[rows, HALF:] = message[place(e), at + SLOT : at + 2 * SLOT, :]


def collector(numbers, gather, rows):
    row = lax.broadcasted_iota(jnp.int32, (STEP, HALF), 0).astype(F32) + float(rows.start)
    for a in range(8):
        gather[:, a * HALF : (a + 1) * HALF] = (row == numbers[a : a + 1, :]).astype(BF16)


def mask_tiles(occupied, local_in, edge_in, cotangent, bank, local, edge, flipped, sem):
    copies = Copies(sem)
    out = [copies.stored(cotangent, bank, "cotangent")]
    tiles = [slice(i * 128, (i + 1) * 128) for i in range(8)]
    for i, rows in enumerate(tiles):
        for j, cols in enumerate(tiles):
            part = local_in[rows, cols]
            local[rows, cols] = jnp.where(occupied[i, j] != 0, part, jnp.zeros_like(part))
    out.append(copies.stored(local, bank, "local"))
    for i, rows in enumerate(tiles):
        for j, cols in enumerate(tiles):
            part = edge_in[rows, cols]
            part = jnp.where(occupied[i, 8 + j] != 0, part, jnp.zeros_like(part))
            edge[rows, cols] = part
            flipped[cols, rows] = part.T
    out += [copies.stored(edge, bank, "edge"), copies.stored(flipped, bank, "flipped")]
    wait(*out)


def serve(me, message, bank, own_x, reply_far, own_h, flipped, reply, sem):
    copies = Copies(sem)
    arriving = [
        copies.start(kept(bank, "flipped", rows), flipped.at[rows]) for rows, peers in steps()
    ]
    take_by_owner(message, 0, own_x)
    take_by_owner(message, 32, own_h)
    wanted = requested(me[0], message[:, 64:72, :]).astype(jnp.int32)
    out = []
    for rows, peers in steps():
        column = lax.broadcasted_iota(jnp.int32, (STEP, ROWS), 1)
        select = (column == wanted[rows]).astype(BF16)
        put(reply, 0, peers, dot(select, own_x[...]).astype(BF16))
        put(reply, 32, peers, dot(select, own_h[...]).astype(BF16))
        out.append(copies.start(reply.at[peers, 0:64], reply_far.at[peers, 0:64]))
    wait(*arriving)
    for rows, peers in steps(STEP // 2):
        put_by_owner(reply, 64, peers, dot(flipped[rows, :], own_x[...]).astype(BF16))
        for part in places(peers):
            out.append(copies.start(reply.at[part, 64:96], reply_far.at[part, 64:96]))
    wait(*out)


def prepare(me, message, own_x, bank, bank_out, numbers, local, high, low, sem):
    copies = Copies(sem)
    first = copies.start(kept(bank, "local", slice(0, ROWS)), local)
    wanted = jnp.broadcast_to(requested(me[0], message[:, 64:72, :]), (ROWS, HALF))
    for a in range(8):
        numbers[a : a + 1, :] = wanted[a * HALF : (a + 1) * HALF].T[0:1, :]
    first.wait()
    for rows, peers in steps():
        total = dot(local[rows, :], own_x[...])
        high[rows, :] = total.astype(BF16)
        low[rows, :] = (total - high[rows, :].astype(F32)).astype(BF16)
    wait(copies.stored(high, bank_out, "high"), copies.stored(low, bank_out, "low"))


def first_layer(
    message, bank, numbers, w, bias, hidden_far, push_far,
    far, pushed, edge, gather, high, low, sums, hidden, push, sem,
):
    copies = Copies(sem)
    into = {"edge": edge, "high": high, "low": low}
    arriving = [
        [copies.start(kept(bank, name, rows), ref.at[rows]) for name, ref in into.items()]
        for rows, peers in steps()
    ]
    take(message, 64, pushed)
    for rows, peers in steps():
        collector(numbers, gather, rows)
        sums[rows, :] = dot(gather[...], pushed[...])
    take_by_owner(message, 0, far)
    for (rows, peers), parts in zip(steps(), arriving):
        wait(*parts)
        total = sums[rows, :] + high[rows, :].astype(F32) + low[rows, :].astype(F32)
        total = total + dot(edge[rows, :], far[...])
        value = dot(total.astype(BF16), w[...]) + bias[...]
        hidden[rows, :] = jnp.maximum(value, 0.0).astype(BF16)
    out = [copies.start(hidden, hidden_far)]
    for rows, peers in steps(STEP // 2):
        put_by_owner(push, 0, peers, dot_flipped(edge[:, rows], hidden[...]).astype(BF16))
        for part in places(peers):
            out.append(copies.start(push.at[part], push_far.at[part]))
    wait(*out)


def second_terms(message, hidden, bank, partial, far, local, edge, sem):
    copies = Copies(sem)
    parts = [
        copies.start(kept(bank, "local", slice(0, ROWS)), local),
        copies.start(kept(bank, "edge", slice(0, ROWS)), edge),
    ]
    take_by_owner(message, 32, far)
    wait(*parts)
    for rows, peers in steps():
        partial[rows, :] = dot(local[rows, :], hidden[...]) + dot(edge[rows, :], far[...])


def second_layer(message, partial, bank, numbers, aggregate, gradient, pushed, gather, cotangent, sem):
    copies = Copies(sem)
    last = copies.start(kept(bank, "cotangent", slice(0, ROWS)), cotangent)
    take(message, 0, pushed)
    for rows, peers in steps():
        collector(numbers, gather, rows)
        total = partial[rows, :] + dot(gather[...], pushed[...])
        aggregate[rows, :] = total.astype(BF16)
    last.wait()
    gradient[...] = lax.dot_general(
        aggregate[...], cotangent[...], (((0,), (0,)), ((), ())), preferred_element_type=F32
    )


def exchange(message):
    return lax.all_to_all(message, ORDER, split_axis=0, concat_axis=0, tiled=True)


def swapped(array, axis, mask):
    return lax.ppermute(array, axis, [(i, i ^ mask) for i in range(lax.axis_size(axis))])


def summed_everywhere(term):
    core = lax.axis_index("dev_2")
    halves = term.reshape(2, ROWS // 8, F)
    kept_half = lax.dynamic_index_in_dim(halves, core, 0, keepdims=False)
    sent = lax.dynamic_index_in_dim(halves, 1 - core, 0, keepdims=False)
    half = (kept_half + swapped(sent, "dev_2", 1)).astype(BF16)
    tiles = lax.all_to_all(half.reshape(32, 4, F), CHIPS, split_axis=0, concat_axis=0, tiled=True)
    own = jnp.sum(tiles.astype(F32), axis=0)
    own = own + swapped(own, "rep", 1)
    own = own + swapped(own, "rep", 3)
    copies = jnp.broadcast_to(own.astype(BF16)[None], (32, 4, F))
    mine = lax.all_to_all(copies, CHIPS, split_axis=0, concat_axis=0, tiled=True).reshape(128, F)
    other = swapped(mine, "dev_2", 1)
    first = jnp.where(core == 0, mine, other)
    second = jnp.where(core == 0, other, mine)
    return jnp.concatenate([first, second], axis=0).astype(F32)


def body(
    features,
    history,
    new_owner,
    pull_rows,
    occupancy,
    adj_local,
    adj_boundary,
    w_first,
    bias_first,
    w_second,
    cotangent,
):
    me = lax.axis_index(DEV).astype(jnp.int32).reshape(1)
    wide = 2 * ROWS * ROWS * F
    nodes, square = pltpu.VMEM((ROWS, F), BF16), pltpu.VMEM((ROWS, ROWS), BF16)
    count = ROWS // STEP

    def letters(rows):
        return pltpu.VMEM((PEERS, rows, HALF), BF16)

    (message,) = call(
        send_clusters,
        "hhhhh",
        (shaped(PEERS, 72, HALF),),
        (new_owner, features, history, pull_rows.reshape(8, 128)),
        own=(
            pltpu.SMEM((1, PEERS), jnp.int32),
            nodes,
            nodes,
            pltpu.VMEM((8, 128), jnp.int32),
            letters(72),
        ),
        copies=6,
        flops=ROWS * F,
        room=0,
        name="send_clusters",
    )
    (bank,) = call(
        mask_tiles,
        "svvvh",
        (shaped(DEPTH, ROWS),),
        (occupancy, adj_local, adj_boundary, cotangent),
        own=(square, square, square),
        copies=4,
        flops=wide,
        name="mask_tiles",
    )
    arrived = exchange(message)
    half = pltpu.VMEM((STEP, ROWS), BF16)
    own_x, reply = call(
        serve,
        "svhvh",
        (shaped(ROWS, F), shaped(PEERS, 96, HALF)),
        (me, arrived, bank),
        own=(nodes, square, letters(96)),
        copies=6 * count,
        flops=3 * wide,
        room=12,
        name="serve",
    )
    bank, numbers = call(
        prepare,
        "svvhhv",
        (shaped(DEPTH, ROWS), shaped(8, HALF, dtype=F32)),
        (me, arrived, own_x, bank),
        own=(square, nodes, nodes),
        copies=3,
        flops=wide,
        alias={3: 0},
        name="prepare",
    )
    answers = exchange(reply)
    hidden, push = call(
        first_layer,
        "vhvvvhh",
        (shaped(ROWS, F), shaped(PEERS, 32, HALF)),
        (answers, bank, numbers, w_first, bias_first.reshape(1, F)),
        own=(
            nodes,
            nodes,
            square,
            half,
            nodes,
            nodes,
            pltpu.VMEM((ROWS, F), F32),
            nodes,
            letters(32),
        ),
        copies=7 * count + 1,
        flops=3 * wide,
        name="first_layer",
    )
    (partial_two,) = call(
        second_terms,
        "vvhv",
        (shaped(ROWS, F, dtype=F32),),
        (answers, hidden, bank),
        own=(nodes, square, square),
        copies=2,
        flops=2 * wide,
        name="second_terms",
    )
    pushed = exchange(push)
    aggregate, term = call(
        second_layer,
        "vvhvvv",
        (shaped(ROWS, F), shaped(F, F, dtype=F32)),
        (pushed, partial_two, bank, numbers),
        own=(nodes, half, nodes),
        copies=1,
        flops=2 * wide,
        name="second_layer",
    )
    output = jnp.dot(aggregate, w_second, preferred_element_type=F32).astype(BF16)
    return (hidden, output, summed_everywhere(term))


def solution(mesh):
    finer = Mesh(
        mesh.devices.reshape(8, 4, 2, mesh.shape["rep"]), ("dev_0", "dev_1", "dev_2", "rep")
    )
    rows = P(DEV_REP, None)
    return jax.shard_map(
        body,
        mesh=finer,
        in_specs=(rows, rows, rows, P(DEV_REP), rows, rows, rows, P(), P(), P(), rows),
        out_specs=(rows, rows, P()),
        check_vma=False,
    )
```

```python
import jax
import jax.numpy as jnp
from jax import lax
from jax.experimental import pallas as pl
from jax.experimental.pallas import tpu as pltpu
from jax.sharding import Mesh
from jax.sharding import PartitionSpec as P

CHIPS = ("dev_0", "dev_1")
DEV = ("dev_0", "dev_1", "dev_2")
ORDER = ("dev_2", "dev_0", "dev_1")
DEV_REP = ("dev_0", "dev_1", "dev_2", "rep")
PEERS, SLOT, HALF, ROWS, F = 64, 16, 128, 1024, 256
STEP = 512
BANK = {
    "local": (0, slice(0, 1024)),
    "edge": (1024, slice(0, 1024)),
    "flipped": (2048, slice(0, 1024)),
    "high": (3072, slice(0, 256)),
    "low": (3072, slice(256, 512)),
    "cotangent": (3072, slice(512, 768)),
}
DEPTH = 4096
VMEM = 67043328

F32, BF16 = jnp.float32, jnp.bfloat16


def dot(a, b):
    return jnp.dot(a, b, preferred_element_type=F32)


def call(body, kinds, outs, operands, *, own=(), copies=0, flops=0, room=16, alias=None, name=None):
    spaces = {"s": pltpu.SMEM, "v": pltpu.VMEM, "h": pltpu.HBM}
    moved = sum(a.size * a.dtype.itemsize for a in (*operands, *outs))
    arrivals = (pltpu.SemaphoreType.DMA((copies,)),) if copies else ()
    specs = [pl.BlockSpec(memory_space=spaces[k]) for k in kinds]
    return pl.pallas_call(
        body,
        out_shape=outs,
        in_specs=specs[: len(operands)],
        out_specs=tuple(specs[len(operands) :]),
        scratch_shapes=(*own, *arrivals),
        input_output_aliases=alias or {},
        compiler_params=pltpu.CompilerParams(vmem_limit_bytes=VMEM - (room << 20)),
        cost_estimate=pl.CostEstimate(flops=flops, bytes_accessed=moved, transcendentals=0),
        name=name,
    )(*operands)


class Copies:
    def __init__(self, semaphores):
        self.semaphores, self.used = semaphores, 0

    def start(self, source, target):
        copy = pltpu.make_async_copy(source, target, self.semaphores.at[self.used])
        self.used += 1
        copy.start()
        return copy

    def stored(self, source, bank, name):
        return self.start(source, kept(bank, name, slice(0, ROWS)))


def kept(bank, name, rows):
    first, columns = BANK[name]
    return bank.at[first + rows.start : first + rows.stop, columns]


def wait(*copies):
    for copy in copies:
        copy.wait()


def dot_flipped(a, b):
    return lax.dot_general(a, b, (((0,), (0,)), ((), ())), preferred_element_type=F32)


def shaped(*dims, dtype=BF16):
    return jax.ShapeDtypeStruct(dims, dtype)


def place(e):
    return (e & 1) * (PEERS // 2) + (e >> 1)


def put(message, at, peers, value):
    count = value.shape[0] // SLOT
    message[peers, at : at + SLOT, :] = value[:, :HALF].reshape(count, SLOT, HALF)
    message[peers, at + SLOT : at + 2 * SLOT, :] = value[:, HALF:].reshape(count, SLOT, HALF)


def put_by_owner(message, at, peers, value):
    for i, e in enumerate(range(peers.start, peers.stop)):
        block = value[i * SLOT : (i + 1) * SLOT]
        message[place(e), at : at + SLOT, :] = block[:, :HALF]
        message[place(e), at + SLOT : at + 2 * SLOT, :] = block[:, HALF:]


def places(peers):
    for core in range(2):
        yield slice(place(peers.start + core), place(peers.stop - 2 + core) + 1)


def steps(step=STEP):
    for at in range(0, ROWS, step):
        yield slice(at, at + step), slice(at // SLOT, (at + step) // SLOT)


def send_clusters(owner, x, h, pulled, message, owners, xs, hs, numbers, packed, sem):
    copies = Copies(sem)
    order = copies.start(owner, owners)
    first = copies.start(x, xs)
    rows_in = copies.start(pulled, numbers)
    second = copies.start(h, hs)
    which = lax.broadcasted_iota(jnp.int32, (8, HALF), 0)
    rows_in.wait()
    for a in range(8):
        line = numbers[a : a + 1, :]
        high = (line // 32).astype(F32)
        low = (line % 32).astype(F32)
        tile = jnp.where(which == 0, high, jnp.where(which == 1, low, 0.0)).astype(BF16)
        for b in range(8):
            packed[place(a * 8 + b), 64:72, :] = tile
    wait(order, first)
    for j in range(PEERS):
        e = place(owners[0, j])
        rows = slice(j * SLOT, (j + 1) * SLOT)
        packed[e, 0:16, :] = xs[rows, :HALF]
        packed[e, 16:32, :] = xs[rows, HALF:]
    out_x = copies.start(packed.at[:, 0:32, :], message.at[:, 0:32, :])
    second.wait()
    for j in range(PEERS):
        e = place(owners[0, j])
        rows = slice(j * SLOT, (j + 1) * SLOT)
        packed[e, 32:48, :] = hs[rows, :HALF]
        packed[e, 48:64, :] = hs[rows, HALF:]
    out_h = copies.start(packed.at[:, 32:72, :], message.at[:, 32:72, :])
    wait(out_x, out_h)


def requested(me, tile):
    tile = tile.astype(F32)
    numbers = 32.0 * tile[:, 0:1, :] + tile[:, 1:2, :]
    lane = lax.broadcasted_iota(jnp.int32, (PEERS, SLOT, HALF), 2)
    place = lax.broadcasted_iota(jnp.int32, (PEERS, SLOT, HALF), 1)
    mine = lane == (me % 8) * SLOT + place
    return jnp.sum(jnp.where(mine, numbers, 0.0), axis=2, keepdims=True).reshape(ROWS, 1)


def take(message, at, into):
    into[:, :HALF] = message[:, at : at + SLOT, :].reshape(ROWS, HALF)
    into[:, HALF:] = message[:, at + SLOT : at + 2 * SLOT, :].reshape(ROWS, HALF)


def take_by_owner(message, at, into):
    for e in range(PEERS):
        rows = slice(e * SLOT, (e + 1) * SLOT)
        into[rows, :HALF] = message[place(e), at : at + SLOT, :]
        into[rows, HALF:] = message[place(e), at + SLOT : at + 2 * SLOT, :]


def collector(numbers, gather, rows):
    row = lax.broadcasted_iota(jnp.int32, (STEP, HALF), 0).astype(F32) + float(rows.start)
    for a in range(8):
        gather[:, a * HALF : (a + 1) * HALF] = (row == numbers[a : a + 1, :]).astype(BF16)


def mask_tiles(occupied, local_in, edge_in, cotangent, bank, local, edge, flipped, sem):
    copies = Copies(sem)
    out = [copies.stored(cotangent, bank, "cotangent")]
    tiles = [slice(i * 128, (i + 1) * 128) for i in range(8)]
    for i, rows in enumerate(tiles):
        for j, cols in enumerate(tiles):
            part = local_in[rows, cols]
            local[rows, cols] = jnp.where(occupied[i, j] != 0, part, jnp.zeros_like(part))
    out.append(copies.stored(local, bank, "local"))
    for i, rows in enumerate(tiles):
        for j, cols in enumerate(tiles):
            part = edge_in[rows, cols]
            part = jnp.where(occupied[i, 8 + j] != 0, part, jnp.zeros_like(part))
            edge[rows, cols] = part
            flipped[cols, rows] = part.T
    out += [copies.stored(edge, bank, "edge"), copies.stored(flipped, bank, "flipped")]
    wait(*out)


def serve(me, message, bank, own_x, reply_far, own_h, flipped, reply, sem):
    copies = Copies(sem)
    arriving = [
        copies.start(kept(bank, "flipped", rows), flipped.at[rows]) for rows, peers in steps()
    ]
    take_by_owner(message, 0, own_x)
    take_by_owner(message, 32, own_h)
    wanted = requested(me[0], message[:, 64:72, :]).astype(jnp.int32)
    out = []
    for rows, peers in steps():
        column = lax.broadcasted_iota(jnp.int32, (STEP, ROWS), 1)
        select = (column == wanted[rows]).astype(BF16)
        put(reply, 0, peers, dot(select, own_x[...]).astype(BF16))
        put(reply, 32, peers, dot(select, own_h[...]).astype(BF16))
        out.append(copies.start(reply.at[peers, 0:64], reply_far.at[peers, 0:64]))
    wait(*arriving)
    for rows, peers in steps(STEP // 2):
        put_by_owner(reply, 64, peers, dot(flipped[rows, :], own_x[...]).astype(BF16))
        for part in places(peers):
            out.append(copies.start(reply.at[part, 64:96], reply_far.at[part, 64:96]))
    wait(*out)


def prepare(me, message, own_x, bank, bank_out, numbers, local, high, low, sem):
    copies = Copies(sem)
    first = copies.start(kept(bank, "local", slice(0, ROWS)), local)
    wanted = jnp.broadcast_to(requested(me[0], message[:, 64:72, :]), (ROWS, HALF))
    for a in range(8):
        numbers[a : a + 1, :] = wanted[a * HALF : (a + 1) * HALF].T[0:1, :]
    first.wait()
    for rows, peers in steps():
        total = dot(local[rows, :], own_x[...])
        high[rows, :] = total.astype(BF16)
        low[rows, :] = (total - high[rows, :].astype(F32)).astype(BF16)
    wait(copies.stored(high, bank_out, "high"), copies.stored(low, bank_out, "low"))


def first_layer(
    message, bank, numbers, w, bias, hidden_far, push_far,
    far, pushed, edge, gather, high, low, sums, hidden, push, sem,
):
    copies = Copies(sem)
    into = {"edge": edge, "high": high, "low": low}
    arriving = [
        [copies.start(kept(bank, name, rows), ref.at[rows]) for name, ref in into.items()]
        for rows, peers in steps()
    ]
    take(message, 64, pushed)
    for rows, peers in steps():
        collector(numbers, gather, rows)
        sums[rows, :] = dot(gather[...], pushed[...])
    take_by_owner(message, 0, far)
    for (rows, peers), parts in zip(steps(), arriving):
        wait(*parts)
        total = sums[rows, :] + high[rows, :].astype(F32) + low[rows, :].astype(F32)
        total = total + dot(edge[rows, :], far[...])
        value = dot(total.astype(BF16), w[...]) + bias[...]
        hidden[rows, :] = jnp.maximum(value, 0.0).astype(BF16)
    out = [copies.start(hidden, hidden_far)]
    for rows, peers in steps(STEP // 2):
        put_by_owner(push, 0, peers, dot_flipped(edge[:, rows], hidden[...]).astype(BF16))
        for part in places(peers):
            out.append(copies.start(push.at[part], push_far.at[part]))
    wait(*out)


def second_terms(message, hidden, bank, partial, far, local, edge, sem):
    copies = Copies(sem)
    parts = [
        copies.start(kept(bank, "local", slice(0, ROWS)), local),
        copies.start(kept(bank, "edge", slice(0, ROWS)), edge),
    ]
    take_by_owner(message, 32, far)
    wait(*parts)
    for rows, peers in steps():
        partial[rows, :] = dot(local[rows, :], hidden[...]) + dot(edge[rows, :], far[...])


def second_layer(
    message, partial, bank, numbers, w, output_far, gradient,
    pushed, gather, cotangent, aggregate, output, sem,
):
    copies = Copies(sem)
    last = copies.start(kept(bank, "cotangent", slice(0, ROWS)), cotangent)
    take(message, 0, pushed)
    out = []
    for rows, peers in steps():
        collector(numbers, gather, rows)
        total = partial[rows, :] + dot(gather[...], pushed[...])
        aggregate[rows, :] = total.astype(BF16)
        output[rows, :] = dot(aggregate[rows, :], w[...]).astype(BF16)
        out.append(copies.start(output.at[rows], output_far.at[rows]))
    last.wait()
    gradient[...] = dot_flipped(aggregate[...], cotangent[...])
    wait(*out)


def exchange(message):
    return lax.all_to_all(message, ORDER, split_axis=0, concat_axis=0, tiled=True)


def swapped(array, axis, mask):
    return lax.ppermute(array, axis, [(i, i ^ mask) for i in range(lax.axis_size(axis))])


def summed_everywhere(term):
    core = lax.axis_index("dev_2")
    halves = term.reshape(2, ROWS // 8, F)
    kept_half = lax.dynamic_index_in_dim(halves, core, 0, keepdims=False)
    sent = lax.dynamic_index_in_dim(halves, 1 - core, 0, keepdims=False)
    half = (kept_half + swapped(sent, "dev_2", 1)).astype(BF16)
    tiles = lax.all_to_all(half.reshape(32, 4, F), CHIPS, split_axis=0, concat_axis=0, tiled=True)
    own = jnp.sum(tiles.astype(F32), axis=0)
    own = (own + swapped(own, "rep", 1)) + (swapped(own, "rep", 2) + swapped(own, "rep", 3))
    copies = jnp.broadcast_to(own.astype(BF16)[None], (32, 4, F))
    mine = lax.all_to_all(copies, CHIPS, split_axis=0, concat_axis=0, tiled=True).reshape(128, F)
    other = swapped(mine, "dev_2", 1)
    first = jnp.where(core == 0, mine, other)
    second = jnp.where(core == 0, other, mine)
    return jnp.concatenate([first, second], axis=0).astype(F32)


def body(
    features,
    history,
    new_owner,
    pull_rows,
    occupancy,
    adj_local,
    adj_boundary,
    w_first,
    bias_first,
    w_second,
    cotangent,
):
    me = lax.axis_index(DEV).astype(jnp.int32).reshape(1)
    wide = 2 * ROWS * ROWS * F
    nodes, square = pltpu.VMEM((ROWS, F), BF16), pltpu.VMEM((ROWS, ROWS), BF16)
    count = ROWS // STEP

    def letters(rows):
        return pltpu.VMEM((PEERS, rows, HALF), BF16)

    (message,) = call(
        send_clusters,
        "hhhhh",
        (shaped(PEERS, 72, HALF),),
        (new_owner, features, history, pull_rows.reshape(8, 128)),
        own=(
            pltpu.SMEM((1, PEERS), jnp.int32),
            nodes,
            nodes,
            pltpu.VMEM((8, 128), jnp.int32),
            letters(72),
        ),
        copies=6,
        flops=ROWS * F,
        room=0,
        name="send_clusters",
    )
    (bank,) = call(
        mask_tiles,
        "svvvh",
        (shaped(DEPTH, ROWS),),
        (occupancy, adj_local, adj_boundary, cotangent),
        own=(square, square, square),
        copies=4,
        flops=wide,
        name="mask_tiles",
    )
    arrived = exchange(message)
    half = pltpu.VMEM((STEP, ROWS), BF16)
    own_x, reply = call(
        serve,
        "svhvh",
        (shaped(ROWS, F), shaped(PEERS, 96, HALF)),
        (me, arrived, bank),
        own=(nodes, square, letters(96)),
        copies=6 * count,
        flops=3 * wide,
        room=12,
        name="serve",
    )
    bank, numbers = call(
        prepare,
        "svvhhv",
        (shaped(DEPTH, ROWS), shaped(8, HALF, dtype=F32)),
        (me, arrived, own_x, bank),
        own=(square, nodes, nodes),
        copies=3,
        flops=wide,
        alias={3: 0},
        name="prepare",
    )
    answers = exchange(reply)
    hidden, push = call(
        first_layer,
        "vhvvvhh",
        (shaped(ROWS, F), shaped(PEERS, 32, HALF)),
        (answers, bank, numbers, w_first, bias_first.reshape(1, F)),
        own=(
            nodes,
            nodes,
            square,
            half,
            nodes,
            nodes,
            pltpu.VMEM((ROWS, F), F32),
            nodes,
            letters(32),
        ),
        copies=7 * count + 1,
        flops=3 * wide,
        name="first_layer",
    )
    (partial_two,) = call(
        second_terms,
        "vvhv",
        (shaped(ROWS, F, dtype=F32),),
        (answers, hidden, bank),
        own=(nodes, square, square),
        copies=2,
        flops=2 * wide,
        name="second_terms",
    )
    pushed = exchange(push)
    output, term = call(
        second_layer,
        "vvhvvhv",
        (shaped(ROWS, F), shaped(F, F, dtype=F32)),
        (pushed, partial_two, bank, numbers, w_second),
        own=(nodes, half, nodes, nodes, nodes),
        copies=1 + count,
        flops=2 * wide,
        name="second_layer",
    )
    return (hidden, output, summed_everywhere(term))


def solution(mesh):
    finer = Mesh(
        mesh.devices.reshape(8, 4, 2, mesh.shape["rep"]), ("dev_0", "dev_1", "dev_2", "rep")
    )
    rows = P(DEV_REP, None)
    return jax.shard_map(
        body,
        mesh=finer,
        in_specs=(rows, rows, rows, P(DEV_REP), rows, rows, rows, P(), P(), P(), rows),
        out_specs=(rows, rows, P()),
        check_vma=False,
    )
```

```python
import jax
import jax.numpy as jnp
from jax import lax
from jax.experimental import pallas as pl
from jax.experimental.pallas import tpu as pltpu
from jax.sharding import Mesh
from jax.sharding import PartitionSpec as P

CHIPS = ("dev_0", "dev_1")
DEV = ("dev_0", "dev_1", "dev_2")
ORDER = ("dev_2", "dev_0", "dev_1")
DEV_REP = ("dev_0", "dev_1", "dev_2", "rep")
PEERS, SLOT, HALF, ROWS, F = 64, 16, 128, 1024, 256
STEP = 512
BANK = {
    "local": (0, slice(0, 1024)),
    "edge": (1024, slice(0, 1024)),
    "flipped": (2048, slice(0, 1024)),
    "high": (3072, slice(0, 256)),
    "low": (3072, slice(256, 512)),
    "cotangent": (3072, slice(512, 768)),
}
DEPTH = 4096
VMEM = 67043328

F32, BF16 = jnp.float32, jnp.bfloat16


def dot(a, b):
    return jnp.dot(a, b, preferred_element_type=F32)


def call(body, kinds, outs, operands, *, own=(), copies=0, flops=0, room=16, alias=None, name=None):
    spaces = {"s": pltpu.SMEM, "v": pltpu.VMEM, "h": pltpu.HBM}
    moved = sum(a.size * a.dtype.itemsize for a in (*operands, *outs))
    arrivals = (pltpu.SemaphoreType.DMA((copies,)),) if copies else ()
    specs = [pl.BlockSpec(memory_space=spaces[k]) for k in kinds]
    return pl.pallas_call(
        body,
        out_shape=outs,
        in_specs=specs[: len(operands)],
        out_specs=tuple(specs[len(operands) :]),
        scratch_shapes=(*own, *arrivals),
        input_output_aliases=alias or {},
        compiler_params=pltpu.CompilerParams(vmem_limit_bytes=VMEM - (room << 20)),
        cost_estimate=pl.CostEstimate(flops=flops, bytes_accessed=moved, transcendentals=0),
        name=name,
    )(*operands)


class Copies:
    def __init__(self, semaphores):
        self.semaphores, self.used = semaphores, 0

    def start(self, source, target):
        copy = pltpu.make_async_copy(source, target, self.semaphores.at[self.used])
        self.used += 1
        copy.start()
        return copy

    def stored(self, source, bank, name):
        return self.start(source, kept(bank, name, slice(0, ROWS)))


def kept(bank, name, rows):
    first, columns = BANK[name]
    return bank.at[first + rows.start : first + rows.stop, columns]


def wait(*copies):
    for copy in copies:
        copy.wait()


def dot_flipped(a, b):
    return lax.dot_general(a, b, (((0,), (0,)), ((), ())), preferred_element_type=F32)


def shaped(*dims, dtype=BF16):
    return jax.ShapeDtypeStruct(dims, dtype)


def place(e):
    return (e & 1) * (PEERS // 2) + (e >> 1)


def put(message, at, peers, value):
    count = value.shape[0] // SLOT
    message[peers, at : at + SLOT, :] = value[:, :HALF].reshape(count, SLOT, HALF)
    message[peers, at + SLOT : at + 2 * SLOT, :] = value[:, HALF:].reshape(count, SLOT, HALF)


def put_by_owner(message, at, peers, value):
    for i, e in enumerate(range(peers.start, peers.stop)):
        block = value[i * SLOT : (i + 1) * SLOT]
        message[place(e), at : at + SLOT, :] = block[:, :HALF]
        message[place(e), at + SLOT : at + 2 * SLOT, :] = block[:, HALF:]


def places(peers):
    for core in range(2):
        yield slice(place(peers.start + core), place(peers.stop - 2 + core) + 1)


def steps(step=STEP):
    for at in range(0, ROWS, step):
        yield slice(at, at + step), slice(at // SLOT, (at + step) // SLOT)


def send_clusters(owner, x, h, pulled, message, owners, xs, hs, numbers, packed, sem):
    copies = Copies(sem)
    order = copies.start(owner, owners)
    first = copies.start(x, xs)
    rows_in = copies.start(pulled, numbers)
    second = copies.start(h, hs)
    which = lax.broadcasted_iota(jnp.int32, (8, HALF), 0)
    rows_in.wait()
    for a in range(8):
        line = numbers[a : a + 1, :]
        high = (line // 32).astype(F32)
        low = (line % 32).astype(F32)
        tile = jnp.where(which == 0, high, jnp.where(which == 1, low, 0.0)).astype(BF16)
        for b in range(8):
            packed[place(a * 8 + b), 64:72, :] = tile
    wait(order, first)
    for j in range(PEERS):
        e = place(owners[0, j])
        rows = slice(j * SLOT, (j + 1) * SLOT)
        packed[e, 0:16, :] = xs[rows, :HALF]
        packed[e, 16:32, :] = xs[rows, HALF:]
    out_x = copies.start(packed.at[:, 0:32, :], message.at[:, 0:32, :])
    second.wait()
    for j in range(PEERS):
        e = place(owners[0, j])
        rows = slice(j * SLOT, (j + 1) * SLOT)
        packed[e, 32:48, :] = hs[rows, :HALF]
        packed[e, 48:64, :] = hs[rows, HALF:]
    out_h = copies.start(packed.at[:, 32:72, :], message.at[:, 32:72, :])
    wait(out_x, out_h)


def requested(me, tile):
    tile = tile.astype(F32)
    numbers = 32.0 * tile[:, 0:1, :] + tile[:, 1:2, :]
    lane = lax.broadcasted_iota(jnp.int32, (PEERS, SLOT, HALF), 2)
    place = lax.broadcasted_iota(jnp.int32, (PEERS, SLOT, HALF), 1)
    mine = lane == (me % 8) * SLOT + place
    return jnp.sum(jnp.where(mine, numbers, 0.0), axis=2, keepdims=True).reshape(ROWS, 1)


def take(message, at, into):
    into[:, :HALF] = message[:, at : at + SLOT, :].reshape(ROWS, HALF)
    into[:, HALF:] = message[:, at + SLOT : at + 2 * SLOT, :].reshape(ROWS, HALF)


def take_by_owner(message, at, into):
    for e in range(PEERS):
        rows = slice(e * SLOT, (e + 1) * SLOT)
        into[rows, :HALF] = message[place(e), at : at + SLOT, :]
        into[rows, HALF:] = message[place(e), at + SLOT : at + 2 * SLOT, :]


def collector(numbers, gather, rows):
    row = lax.broadcasted_iota(jnp.int32, (STEP, HALF), 0).astype(F32) + float(rows.start)
    for a in range(8):
        gather[:, a * HALF : (a + 1) * HALF] = (row == numbers[a : a + 1, :]).astype(BF16)


def mask_tiles(occupied, local_in, edge_in, cotangent, bank, local, edge, flipped, sem):
    copies = Copies(sem)
    out = [copies.stored(cotangent, bank, "cotangent")]
    tiles = [slice(i * 128, (i + 1) * 128) for i in range(8)]
    for i, rows in enumerate(tiles):
        for j, cols in enumerate(tiles):
            part = local_in[rows, cols]
            local[rows, cols] = jnp.where(occupied[i, j] != 0, part, jnp.zeros_like(part))
    out.append(copies.stored(local, bank, "local"))
    for i, rows in enumerate(tiles):
        for j, cols in enumerate(tiles):
            part = edge_in[rows, cols]
            part = jnp.where(occupied[i, 8 + j] != 0, part, jnp.zeros_like(part))
            edge[rows, cols] = part
            flipped[cols, rows] = part.T
    out += [copies.stored(edge, bank, "edge"), copies.stored(flipped, bank, "flipped")]
    wait(*out)


def serve(me, message, bank, own_x, reply_far, own_h, flipped, reply, sem):
    copies = Copies(sem)
    arriving = [
        copies.start(kept(bank, "flipped", rows), flipped.at[rows]) for rows, peers in steps()
    ]
    take_by_owner(message, 0, own_x)
    take_by_owner(message, 32, own_h)
    wanted = requested(me[0], message[:, 64:72, :]).astype(jnp.int32)
    out = []
    for rows, peers in steps():
        column = lax.broadcasted_iota(jnp.int32, (STEP, ROWS), 1)
        select = (column == wanted[rows]).astype(BF16)
        put(reply, 0, peers, dot(select, own_x[...]).astype(BF16))
        put(reply, 32, peers, dot(select, own_h[...]).astype(BF16))
        out.append(copies.start(reply.at[peers, 0:64], reply_far.at[peers, 0:64]))
    wait(*arriving)
    for rows, peers in steps(STEP // 2):
        put_by_owner(reply, 64, peers, dot(flipped[rows, :], own_x[...]).astype(BF16))
        for part in places(peers):
            out.append(copies.start(reply.at[part, 64:96], reply_far.at[part, 64:96]))
    wait(*out)


def prepare(me, message, own_x, bank, bank_out, numbers, local, high, low, sem):
    copies = Copies(sem)
    first = copies.start(kept(bank, "local", slice(0, ROWS)), local)
    wanted = jnp.broadcast_to(requested(me[0], message[:, 64:72, :]), (ROWS, HALF))
    for a in range(8):
        numbers[a : a + 1, :] = wanted[a * HALF : (a + 1) * HALF].T[0:1, :]
    first.wait()
    for rows, peers in steps():
        total = dot(local[rows, :], own_x[...])
        high[rows, :] = total.astype(BF16)
        low[rows, :] = (total - high[rows, :].astype(F32)).astype(BF16)
    wait(copies.stored(high, bank_out, "high"), copies.stored(low, bank_out, "low"))


def first_layer(
    message, bank, numbers, w, bias, hidden_far, push_far,
    far, pushed, edge, gather, high, low, sums, hidden, push, sem,
):
    copies = Copies(sem)
    into = {"edge": edge, "high": high, "low": low}
    arriving = [
        [copies.start(kept(bank, name, rows), ref.at[rows]) for name, ref in into.items()]
        for rows, peers in steps()
    ]
    take(message, 64, pushed)
    for rows, peers in steps():
        collector(numbers, gather, rows)
        sums[rows, :] = dot(gather[...], pushed[...])
    take_by_owner(message, 0, far)
    for (rows, peers), parts in zip(steps(), arriving):
        wait(*parts)
        total = sums[rows, :] + high[rows, :].astype(F32) + low[rows, :].astype(F32)
        total = total + dot(edge[rows, :], far[...])
        value = dot(total.astype(BF16), w[...]) + bias[...]
        hidden[rows, :] = jnp.maximum(value, 0.0).astype(BF16)
    out = [copies.start(hidden, hidden_far)]
    for rows, peers in steps(STEP // 2):
        put_by_owner(push, 0, peers, dot_flipped(edge[:, rows], hidden[...]).astype(BF16))
        for part in places(peers):
            out.append(copies.start(push.at[part], push_far.at[part]))
    wait(*out)


def second_terms(message, hidden, bank, partial, far, local, edge, sem):
    copies = Copies(sem)
    parts = [
        copies.start(kept(bank, "local", slice(0, ROWS)), local),
        copies.start(kept(bank, "edge", slice(0, ROWS)), edge),
    ]
    take_by_owner(message, 32, far)
    wait(*parts)
    for rows, peers in steps():
        partial[rows, :] = dot(local[rows, :], hidden[...]) + dot(edge[rows, :], far[...])


def second_layer(
    message, partial, bank, numbers, w, output_far, gradient,
    pushed, gather, cotangent, aggregate, output, sem,
):
    copies = Copies(sem)
    last = copies.start(kept(bank, "cotangent", slice(0, ROWS)), cotangent)
    take(message, 0, pushed)
    out = []
    for rows, peers in steps():
        collector(numbers, gather, rows)
        total = partial[rows, :] + dot(gather[...], pushed[...])
        aggregate[rows, :] = total.astype(BF16)
        output[rows, :] = dot(aggregate[rows, :], w[...]).astype(BF16)
        out.append(copies.start(output.at[rows], output_far.at[rows]))
    last.wait()
    gradient[...] = dot_flipped(aggregate[...], cotangent[...])
    wait(*out)


def exchange(message):
    return lax.all_to_all(message, ORDER, split_axis=0, concat_axis=0, tiled=True)


def swapped(array, axis, mask):
    return lax.ppermute(array, axis, [(i, i ^ mask) for i in range(lax.axis_size(axis))])


def summed_everywhere(term):
    core = lax.axis_index("dev_2")
    halves = term.reshape(2, ROWS // 8, F)
    kept_half = lax.dynamic_index_in_dim(halves, core, 0, keepdims=False)
    sent = lax.dynamic_index_in_dim(halves, 1 - core, 0, keepdims=False)
    half = (kept_half + swapped(sent.astype(BF16), "dev_2", 1)).astype(BF16)
    tiles = lax.all_to_all(half.reshape(32, 4, F), CHIPS, split_axis=0, concat_axis=0, tiled=True)
    own = jnp.sum(tiles.astype(F32), axis=0)
    own = (own + swapped(own, "rep", 1)) + (swapped(own, "rep", 2) + swapped(own, "rep", 3))
    copies = jnp.broadcast_to(own.astype(BF16)[None], (32, 4, F))
    mine = lax.all_to_all(copies, CHIPS, split_axis=0, concat_axis=0, tiled=True).reshape(128, F)
    other = swapped(mine, "dev_2", 1)
    first = jnp.where(core == 0, mine, other)
    second = jnp.where(core == 0, other, mine)
    return jnp.concatenate([first, second], axis=0).astype(F32)


def body(
    features,
    history,
    new_owner,
    pull_rows,
    occupancy,
    adj_local,
    adj_boundary,
    w_first,
    bias_first,
    w_second,
    cotangent,
):
    me = lax.axis_index(DEV).astype(jnp.int32).reshape(1)
    wide = 2 * ROWS * ROWS * F
    nodes, square = pltpu.VMEM((ROWS, F), BF16), pltpu.VMEM((ROWS, ROWS), BF16)
    count = ROWS // STEP

    def letters(rows):
        return pltpu.VMEM((PEERS, rows, HALF), BF16)

    (message,) = call(
        send_clusters,
        "hhhhh",
        (shaped(PEERS, 72, HALF),),
        (new_owner, features, history, pull_rows.reshape(8, 128)),
        own=(
            pltpu.SMEM((1, PEERS), jnp.int32),
            nodes,
            nodes,
            pltpu.VMEM((8, 128), jnp.int32),
            letters(72),
        ),
        copies=6,
        flops=ROWS * F,
        room=0,
        name="send_clusters",
    )
    (bank,) = call(
        mask_tiles,
        "svvvh",
        (shaped(DEPTH, ROWS),),
        (occupancy, adj_local, adj_boundary, cotangent),
        own=(square, square, square),
        copies=4,
        flops=wide,
        name="mask_tiles",
    )
    arrived = exchange(message)
    half = pltpu.VMEM((STEP, ROWS), BF16)
    own_x, reply = call(
        serve,
        "svhvh",
        (shaped(ROWS, F), shaped(PEERS, 96, HALF)),
        (me, arrived, bank),
        own=(nodes, square, letters(96)),
        copies=6 * count,
        flops=3 * wide,
        room=12,
        name="serve",
    )
    bank, numbers = call(
        prepare,
        "svvhhv",
        (shaped(DEPTH, ROWS), shaped(8, HALF, dtype=F32)),
        (me, arrived, own_x, bank),
        own=(square, nodes, nodes),
        copies=3,
        flops=wide,
        alias={3: 0},
        name="prepare",
    )
    answers = exchange(reply)
    hidden, push = call(
        first_layer,
        "vhvvvhh",
        (shaped(ROWS, F), shaped(PEERS, 32, HALF)),
        (answers, bank, numbers, w_first, bias_first.reshape(1, F)),
        own=(
            nodes,
            nodes,
            square,
            half,
            nodes,
            nodes,
            pltpu.VMEM((ROWS, F), F32),
            nodes,
            letters(32),
        ),
        copies=7 * count + 1,
        flops=3 * wide,
        name="first_layer",
    )
    (partial_two,) = call(
        second_terms,
        "vvhv",
        (shaped(ROWS, F, dtype=F32),),
        (answers, hidden, bank),
        own=(nodes, square, square),
        copies=2,
        flops=2 * wide,
        name="second_terms",
    )
    pushed = exchange(push)
    output, term = call(
        second_layer,
        "vvhvvhv",
        (shaped(ROWS, F), shaped(F, F, dtype=F32)),
        (pushed, partial_two, bank, numbers, w_second),
        own=(nodes, half, nodes, nodes, nodes),
        copies=1 + count,
        flops=2 * wide,
        name="second_layer",
    )
    return (hidden, output, summed_everywhere(term))


def solution(mesh):
    finer = Mesh(
        mesh.devices.reshape(8, 4, 2, mesh.shape["rep"]), ("dev_0", "dev_1", "dev_2", "rep")
    )
    rows = P(DEV_REP, None)
    return jax.shard_map(
        body,
        mesh=finer,
        in_specs=(rows, rows, rows, P(DEV_REP), rows, rows, rows, P(), P(), P(), rows),
        out_specs=(rows, rows, P()),
        check_vma=False,
    )
```
